32 devices in a mesh: layer: 4 (over x, core), grid: 8 (over z, y).
Axes of the slice: x: 2, y: 2, z: 4, core: 2. Of those that a mesh axis runs over, the one named last changes fastest.
Arguments:
- fourier: float32 [1024, 512, 256], P(('layer', 'grid')), may hold values from -6 to 6
- weights: float32 [1024], P(('layer', 'grid')), may hold values from 0.009375 to 0.09375
- legendre: float32 [256, 513, 1024], P('grid'), may hold values from -6 to 6
- pair_slots: int32 [256], replicated, may hold values from 0 to 255, each once
Outputs:
- spectra: float32 [256, 513, 256], P('grid', None, 'layer')
The draws below stay inside these ranges and needn't reach their ends.
Inputs may be any that keep to these rules, and one draw needn't show every extreme that they name: Each pair index appears exactly once; position q holds wavenumbers pair_slots[q] and 511 - pair_slots[q].
All inputs are finite; a program needn't handle non-finite values.
Results may differ from the reference program's by a relative error of at most 0.0003.
Values sent between devices are 32-bit elements; how exact they have to be, the bound alone decides.
A program may use at most 256 MiB of HBM per device.

```python
import math
import jax
import jax.numpy as jnp
from jax import lax

M = 512
J = 1024
C = 256
PAIRS = 256


def steps_of(rng, extent, shards, low, top_value):
    gain, own = 1.0, jax.random.fold_in(rng, 6)
    for position, shards_of in shards:
        steps = jnp.exp(jax.random.uniform(jax.random.fold_in(own, position), (shards_of,), jnp.float32, low / len(shards), top_value / len(shards)))
        gain = gain * jnp.repeat(steps, extent[position] // shards_of).reshape([-1 if axis == position else 1 for axis in range(len(extent))])
    return gain


def normal_values(own_key, extent, scale, reach, cuts=(), kind=jnp.bfloat16):
    values = scale * jax.random.normal(own_key, extent, jnp.float32)
    if cuts:
        values = values * steps_of(own_key, extent, cuts, -0.22, 0.18)
    return jnp.clip(values, -reach, reach).astype(kind)


def setup_inputs(seed: int = 0) -> dict:
    keys = jax.random.split(jax.random.key(seed), 5)
    fourier = normal_values(keys[0], (J, M, C), 1.0, 6.0, ((0, 32),), jnp.float32)
    weights = jnp.clip(jnp.exp(math.log(0.09375) - 2.3025851 * jax.random.uniform(keys[1], (J,), jnp.float32) ** steps_of(keys[1], (J,), ((0, 32),), -0.2, 0.2)), 0.009375, 0.09375)
    legendre = normal_values(keys[2], (PAIRS, M + 1, J), 1.0, 6.0, ((0, 8),), jnp.float32)
    pair_slots = jax.random.permutation(keys[3], PAIRS).astype(jnp.int32)
    return dict(fourier=fourier, weights=weights, legendre=legendre, pair_slots=pair_slots)


def reference(fourier, weights, legendre, pair_slots):
    scaled = fourier * weights[:, None, None]
    row_ids = jnp.arange(M + 1, dtype=jnp.int32)
    fields_count = scaled.shape[2]

    def pair_block(inputs):
        poly_block, slot_value = inputs
        wave_first = slot_value.astype(jnp.int32)
        wave_second = (M - 1 - slot_value).astype(jnp.int32)
        first_values = lax.dynamic_index_in_dim(scaled, wave_first, 1, keepdims=False)
        second_values = lax.dynamic_index_in_dim(scaled, wave_second, 1, keepdims=False)
        stacked = jnp.concatenate([first_values, second_values], axis=1)
        product = jnp.dot(poly_block, stacked, precision=lax.Precision.HIGHEST, preferred_element_type=jnp.float32)
        in_first = row_ids[:, None] < (M - wave_first)
        return jnp.where(in_first, product[:, :fields_count], product[:, fields_count:])

    return lax.map(pair_block, (legendre, pair_slots))
```

```python
import functools

import jax
import jax.numpy as jnp
from jax import lax
from jax.experimental import pallas as pl
from jax.experimental.pallas import tpu as pltpu
from jax.sharding import PartitionSpec as P

LANES = 128
SUBLANES = 8
MESH = pl.DeviceIdType.MESH


def split(x):
    high = x.astype(jnp.bfloat16)
    return high, (x - high.astype(jnp.float32)).astype(jnp.bfloat16)


def transform_kernel(
    layers, grids, waves, lats, chunk, ahead,
    slots_ref, w_ref, x_ref, poly_ref,
    o_ref, send_ref, recv_ref,
    scale, stage, poly, fields, result,
    load_sem, stage_sem, send_sem, recv_sem, poly_sem, field_sem, out_sem, *held,
):
    devices = layers * grids
    tiles, pitch = lats // SUBLANES, held[0].shape[0] // SUBLANES
    columns = len(held) // tiles
    local_pairs, half, degrees = o_ref.shape
    chunks = local_pairs // chunk
    per_group = SUBLANES // chunk
    my_layer, my_grid = lax.axis_index("layer"), lax.axis_index("grid")
    me = my_layer * grids + my_grid

    def loads(column, tile):
        for row in range(SUBLANES):
            yield pltpu.make_async_copy(
                x_ref.at[pl.ds((tile * SUBLANES + row) * waves, waves), pl.ds(column * LANES, LANES)],
                held[column * tiles + tile].at[pl.ds(row * pitch, waves)],
                load_sem.at[column, tile, row],
            )

    def poly_copies(group):
        rows = pl.ds(pl.multiple_of(group * SUBLANES, SUBLANES), SUBLANES)
        for part in range(poly.shape[0]):
            yield pltpu.make_async_copy(
                poly_ref.at[:, rows, pl.ds(part * LANES, LANES)],
                poly.at[part, pl.ds(0, degrees)],
                poly_sem.at[part],
            )

    def whole(ref, index, sem):
        block = ref.at[index, pl.ds(0, devices - 1)]
        return pltpu.make_async_copy(block, block, sem.at[index])

    for tile in range(tiles):
        for column in range(columns):
            for copy in loads(column, tile):
                copy.start()

    barrier = pltpu.get_barrier_semaphore()

    def greet(step, carry):
        other = lax.rem(me + step, devices)
        pl.semaphore_signal(
            barrier, inc=1, device_id=(other // grids, lax.rem(other, grids)), device_id_type=MESH
        )
        return carry

    lax.fori_loop(1, devices, greet, 0)

    row_ids = lax.broadcasted_iota(jnp.int32, (SUBLANES, LANES), 0)
    for tile in range(tiles):
        value = jnp.zeros((SUBLANES, LANES), jnp.float32)
        for row in range(SUBLANES):
            value = jnp.where(row_ids == row, w_ref[tile * SUBLANES + row], value)
        scale[tile] = value
    parts, rows = poly.shape[0], poly.shape[1]
    for part in range(parts):
        poly[part, pl.ds(degrees, rows - degrees)] = jnp.zeros((rows - degrees, SUBLANES, LANES), jnp.float32)

    in_low = lax.broadcasted_iota(jnp.int32, (SUBLANES, LANES), 1) < half

    def pack(index, first):
        for tile in range(tiles):
            for column in range(columns):
                if first:
                    for copy in loads(column, tile):
                        copy.wait()
                x = held[column * tiles + tile]
                weight = scale[tile]

                def step(q, carry):
                    grid, place = q // chunk, lax.rem(q, chunk)
                    a = slots_ref[grid * local_pairs + index * chunk + place]
                    one = x[pl.ds(a, SUBLANES, stride=pitch), :] * weight
                    two = x[pl.ds(waves - 1 - a, SUBLANES, stride=pitch), :] * weight
                    lower, upper = 2 * column * grids + grid, (2 * column + 1) * grids + grid
                    rows = pl.ds(tile * SUBLANES, SUBLANES)
                    stage[lower, place, rows] = jnp.where(in_low, one, pltpu.roll(two, half, 1))
                    stage[upper, place, rows] = jnp.where(in_low, pltpu.roll(one, half, 1), two)
                    return carry

                lax.fori_loop(0, grids * chunk, step, 0, unroll=8)
        out = pltpu.make_async_copy(stage, send_ref.at[index], stage_sem.at[0])
        own = pltpu.make_async_copy(stage.at[me], recv_ref.at[index, me], stage_sem.at[1])
        out.start()
        own.start()
        out.wait()
        own.wait()

    def send(index):
        def step(k, carry):
            other = lax.rem(me + k, devices)
            pltpu.make_async_remote_copy(
                src_ref=send_ref.at[index, other],
                dst_ref=recv_ref.at[index, me],
                send_sem=send_sem.at[index],
                recv_sem=recv_sem.at[index],
                device_id=(other // grids, lax.rem(other, grids)),
                device_id_type=MESH,
            ).start()
            return carry

        lax.fori_loop(1, devices, step, 0)

    pack(0, True)
    pl.semaphore_wait(barrier, devices - 1)
    send(0)
    for copy in poly_copies(0):
        copy.start()

    def prepare(index, carry):
        pack(index, False)
        send(index)
        return carry

    lax.fori_loop(1, ahead, prepare, 0)

    def consume(index, carry):
        @pl.when(index + ahead < chunks)
        def _():
            prepare(index + ahead, 0)

        group, place = index // per_group, lax.rem(index, per_group)

        @pl.when(place == 0)
        def _():
            for copy in poly_copies(group):
                copy.wait()

        whole(recv_ref, index, recv_sem).wait()
        copy = pltpu.make_async_copy(recv_ref.at[index], fields, field_sem)
        copy.start()
        copy.wait()

        def pair(p, carry):
            limit = waves - slots_ref[my_grid * local_pairs + index * chunk + p]
            x = fields[:, pl.ds(p, 1)].reshape(devices * lats, LANES)
            right = jnp.concatenate(split(x), axis=1)
            spots = pl.ds(place * chunk + p, rows, stride=SUBLANES)
            left = [poly.at[part].reshape(rows * SUBLANES, LANES)[spots, :] for part in range(parts)]
            high, low = split(jnp.concatenate(left, axis=1))
            product = jnp.dot(high, right, preferred_element_type=jnp.float32)
            product = product + jnp.dot(low, right, preferred_element_type=jnp.float32)
            total = (product[:, :LANES] + product[:, LANES:]).T
            ids = lax.broadcasted_iota(jnp.int32, (half, rows), 1)
            result[p] = jnp.where(ids < limit, total[:half], total[half:])[:, :degrees]
            return carry

        lax.fori_loop(0, chunk, pair, 0)

        @pl.when((place == per_group - 1) & (index + 1 < chunks))
        def _():
            for copy in poly_copies(group + 1):
                copy.start()

        copy = pltpu.make_async_copy(result, o_ref.at[pl.ds(index * chunk, chunk)], out_sem)
        copy.start()
        copy.wait()
        return carry

    lax.fori_loop(0, chunks, consume, 0)

    def finish(index, carry):
        whole(send_ref, index, send_sem).wait()
        return carry

    lax.fori_loop(0, chunks, finish, 0)


def shards(layers, grids, fourier, weights, legendre, pair_slots):
    local_pairs, degrees, all_lats = legendre.shape
    waves = 2 * pair_slots.shape[0]
    lats, _, all_fields = fourier.shape
    half = all_fields // layers
    devices = layers * grids
    chunk = 2
    chunks = local_pairs // chunk
    ahead = min(3, chunks)
    rows = (degrees + SUBLANES - 1) // SUBLANES * SUBLANES
    columns, tiles, pitch = all_fields // LANES, lats // SUBLANES, waves + SUBLANES
    block = (devices, chunk, lats, LANES)
    hbm = pl.BlockSpec(memory_space=pl.ANY)
    smem = pl.BlockSpec(memory_space=pltpu.SMEM)
    out = pl.pallas_call(
        functools.partial(transform_kernel, layers, grids, waves, lats, chunk, ahead),
        in_specs=[smem, smem, hbm, hbm],
        out_specs=[hbm, hbm, hbm],
        out_shape=[
            jax.ShapeDtypeStruct((local_pairs, half, degrees), jnp.float32),
            jax.ShapeDtypeStruct((chunks,) + block, jnp.float32),
            jax.ShapeDtypeStruct((chunks,) + block, jnp.float32),
        ],
        scratch_shapes=[
            pltpu.VMEM((tiles, SUBLANES, LANES), jnp.float32),
            pltpu.VMEM(block, jnp.float32),
            pltpu.VMEM((all_lats // LANES, rows, SUBLANES, LANES), jnp.float32),
            pltpu.VMEM(block, jnp.float32),
            pltpu.VMEM((chunk, half, degrees), jnp.float32),
            pltpu.SemaphoreType.DMA((columns, tiles, SUBLANES)),
            pltpu.SemaphoreType.DMA((2,)),
            pltpu.SemaphoreType.DMA((chunks,)),
            pltpu.SemaphoreType.DMA((chunks,)),
            pltpu.SemaphoreType.DMA((all_lats // LANES,)),
            pltpu.SemaphoreType.DMA,
            pltpu.SemaphoreType.DMA,
        ]
        + [pltpu.VMEM((SUBLANES * pitch, LANES), jnp.float32)] * (columns * tiles),
        compiler_params=pltpu.CompilerParams(
            collective_id=0, has_side_effects=True, vmem_limit_bytes=60 * 2**20
        ),
        name="transform",
    )(pair_slots, weights, fourier.reshape(lats * waves, all_fields), legendre.transpose(1, 0, 2))[0]
    return out.transpose(0, 2, 1)


def solution(mesh):
    in_specs = (P(("layer", "grid"), None, None), P(("layer", "grid")), P("grid", None, None), P())
    out_specs = P("grid", None, "layer")
    body = functools.partial(shards, mesh.shape["layer"], mesh.shape["grid"])
    return jax.shard_map(body, mesh=mesh, in_specs=in_specs, out_specs=out_specs, check_vma=False)
```

```python
import functools

import jax
import jax.numpy as jnp
from jax import lax
from jax.experimental import pallas as pl
from jax.experimental.pallas import tpu as pltpu
from jax.sharding import PartitionSpec as P

LANES = 128
SUBLANES = 8
MESH = pl.DeviceIdType.MESH


def split(x):
    high = x.astype(jnp.bfloat16)
    return high, (x - high.astype(jnp.float32)).astype(jnp.bfloat16)


def transform_kernel(
    layers, grids, waves, lats, chunk, ahead,
    slots_ref, w_ref, x_ref, poly_ref,
    o_ref, send_ref, recv_ref,
    scale, stage, poly, fields, result,
    load_sem, stage_sem, send_sem, recv_sem, poly_sem, field_sem, out_sem, *held,
):
    devices = layers * grids
    tiles, pitch = lats // SUBLANES, held[0].shape[0] // SUBLANES
    columns = len(held) // tiles
    local_pairs, half, degrees = o_ref.shape
    chunks = local_pairs // chunk
    per_group = SUBLANES // chunk
    my_layer, my_grid = lax.axis_index("layer"), lax.axis_index("grid")
    me = my_layer * grids + my_grid

    def loads(column, tile):
        for row in range(SUBLANES):
            yield pltpu.make_async_copy(
                x_ref.at[pl.ds((tile * SUBLANES + row) * waves, waves), pl.ds(column * LANES, LANES)],
                held[column * tiles + tile].at[pl.ds(row * pitch, waves)],
                load_sem.at[column, tile, row],
            )

    def poly_copies(group):
        rows = pl.ds(pl.multiple_of(group * SUBLANES, SUBLANES), SUBLANES)
        for part in range(poly.shape[0]):
            yield pltpu.make_async_copy(
                poly_ref.at[:, rows, pl.ds(part * LANES, LANES)],
                poly.at[part, pl.ds(0, degrees)],
                poly_sem.at[part],
            )

    def whole(ref, index, sem):
        block = ref.at[index, pl.ds(0, devices - 1)]
        return pltpu.make_async_copy(block, block, sem.at[index])

    for tile in range(tiles):
        for column in range(columns):
            for copy in loads(column, tile):
                copy.start()

    barrier = pltpu.get_barrier_semaphore()

    def greet(step, carry):
        other = lax.rem(me + step, devices)
        pl.semaphore_signal(
            barrier, inc=1, device_id=(other // grids, lax.rem(other, grids)), device_id_type=MESH
        )
        return carry

    lax.fori_loop(1, devices, greet, 0)

    row_ids = lax.broadcasted_iota(jnp.int32, (SUBLANES, LANES), 0)
    for tile in range(tiles):
        value = jnp.zeros((SUBLANES, LANES), jnp.float32)
        for row in range(SUBLANES):
            value = jnp.where(row_ids == row, w_ref[tile * SUBLANES + row], value)
        scale[tile] = value
    parts, rows = poly.shape[0], poly.shape[1]
    for part in range(parts):
        poly[part, pl.ds(degrees, rows - degrees)] = jnp.zeros((rows - degrees, SUBLANES, LANES), jnp.float32)

    in_low = lax.broadcasted_iota(jnp.int32, (SUBLANES, LANES), 1) < half

    def pack(index, first):
        for tile in range(tiles):
            for column in range(columns):
                if first:
                    for copy in loads(column, tile):
                        copy.wait()
                x = held[column * tiles + tile]
                weight = scale[tile]

                def step(q, carry):
                    grid, place = q // chunk, lax.rem(q, chunk)
                    a = slots_ref[grid * local_pairs + index * chunk + place]
                    one = x[pl.ds(a, SUBLANES, stride=pitch), :] * weight
                    two = x[pl.ds(waves - 1 - a, SUBLANES, stride=pitch), :] * weight
                    lower, upper = 2 * column * grids + grid, (2 * column + 1) * grids + grid
                    rows = pl.ds(tile * SUBLANES, SUBLANES)
                    stage[lower, place, rows] = jnp.where(in_low, one, pltpu.roll(two, half, 1))
                    stage[upper, place, rows] = jnp.where(in_low, pltpu.roll(one, half, 1), two)
                    return carry

                lax.fori_loop(0, grids * chunk, step, 0, unroll=8)
        out = pltpu.make_async_copy(stage, send_ref.at[index], stage_sem.at[0])
        own = pltpu.make_async_copy(stage.at[me], recv_ref.at[index, me], stage_sem.at[1])
        out.start()
        own.start()
        out.wait()
        own.wait()

    def send(index):
        def step(k, carry):
            other = lax.rem(me + k, devices)
            pltpu.make_async_remote_copy(
                src_ref=send_ref.at[index, other],
                dst_ref=recv_ref.at[index, me],
                send_sem=send_sem.at[index],
                recv_sem=recv_sem.at[index],
                device_id=(other // grids, lax.rem(other, grids)),
                device_id_type=MESH,
            ).start()
            return carry

        lax.fori_loop(1, devices, step, 0)

    pack(0, True)
    pl.semaphore_wait(barrier, devices - 1)
    send(0)
    for copy in poly_copies(0):
        copy.start()

    def prepare(index, carry):
        pack(index, False)
        send(index)
        return carry

    lax.fori_loop(1, ahead, prepare, 0)

    def consume(index, carry):
        @pl.when(index + ahead < chunks)
        def _():
            prepare(index + ahead, 0)

        group, place = index // per_group, lax.rem(index, per_group)

        @pl.when(place == 0)
        def _():
            for copy in poly_copies(group):
                copy.wait()

        whole(recv_ref, index, recv_sem).wait()
        copy = pltpu.make_async_copy(recv_ref.at[index], fields, field_sem)
        copy.start()
        copy.wait()

        def pair(p, carry):
            limit = waves - slots_ref[my_grid * local_pairs + index * chunk + p]
            x = fields[:, pl.ds(p, 1)].reshape(devices * lats, LANES)
            right = jnp.concatenate(split(x), axis=1)
            spots = pl.ds(place * chunk + p, rows, stride=SUBLANES)
            left = [poly.at[part].reshape(rows * SUBLANES, LANES)[spots, :] for part in range(parts)]
            high, low = split(jnp.concatenate(left, axis=1))
            product = jnp.dot(high, right, preferred_element_type=jnp.float32)
            product = product + jnp.dot(low, right, preferred_element_type=jnp.float32)
            total = (product[:, :LANES] + product[:, LANES:]).T
            ids = lax.broadcasted_iota(jnp.int32, (half, rows), 1)
            result[p] = jnp.where(ids < limit, total[:half], total[half:])[:, :degrees]
            return carry

        lax.fori_loop(0, chunk, pair, 0)

        @pl.when((place == per_group - 1) & (index + 1 < chunks))
        def _():
            for copy in poly_copies(group + 1):
                copy.start()

        copy = pltpu.make_async_copy(result, o_ref.at[pl.ds(index * chunk, chunk)], out_sem)
        copy.start()
        copy.wait()
        return carry

    lax.fori_loop(0, chunks, consume, 0)

    def finish(index, carry):
        whole(send_ref, index, send_sem).wait()
        return carry

    lax.fori_loop(0, chunks, finish, 0)

def plan_kernel(waves, caps, slots_ref, table_ref, flag_ref):
    grids, local_pairs = slots_ref.shape
    dropped = 2 * len(caps)
    a = slots_ref[...]
    b = waves - 1 - a
    lane = lax.broadcasted_iota(jnp.int32, a.shape, 1)
    zero = jnp.zeros_like(a)
    rank = zero
    for p in range(local_pairs):
        rank = rank + jnp.where(a[:, p : p + 1] < a, 1, 0)
    kept = jnp.where(rank < dropped, 0, 1)
    place = zero
    for p in range(local_pairs):
        place = place + jnp.where(lane > p, kept[:, p : p + 1], 0)
    listed, gone, spot = zero, zero, zero
    for p in range(local_pairs):
        wave = b[:, p : p + 1]
        listed = listed + jnp.where((lane == place[:, p : p + 1]) & (kept[:, p : p + 1] == 1), wave, 0)
        mine = (lane == rank[:, p : p + 1]) & (lane < dropped)
        gone = gone + jnp.where(mine, wave, 0)
        spot = spot + jnp.where(mine, p, 0)
    cap = zero + waves
    for index, value in enumerate(caps):
        cap = jnp.where((lane // 2) == index, value, cap)
    fits = jnp.where((lane < dropped) & (waves - gone > cap), 1.0, 0.0)
    flag_ref[0] = (jnp.sum(fits) < 0.5).astype(jnp.int32)
    place = jnp.where(kept == 1, place, 0)
    rank = jnp.where(kept == 1, 0, rank)
    for index, value in enumerate(
        (a, listed, gone, spot, place // 2, lax.rem(place, 2), kept, rank // 2, lax.rem(rank, 2))
    ):
        table_ref[pl.ds(index * grids, grids)] = value


SLOT, LISTED, GONE, SPOT, LIST_TILE, LIST_SIDE, KEPT, RANK_TILE, RANK_SIDE = range(9)


def plan(pair_slots, grids, waves, caps):
    slots = pair_slots.reshape(grids, -1)
    return pl.pallas_call(
        functools.partial(plan_kernel, waves, caps),
        in_specs=[pl.BlockSpec(memory_space=pltpu.VMEM)],
        out_specs=[pl.BlockSpec(memory_space=pltpu.VMEM), pl.BlockSpec(memory_space=pltpu.SMEM)],
        out_shape=[
            jax.ShapeDtypeStruct((9 * grids, slots.shape[1]), jnp.int32),
            jax.ShapeDtypeStruct((1,), jnp.int32),
        ],
        name="plan",
    )(slots)


def shared_kernel(
    layers, grids, waves, lats, caps, ahead, stops,
    table_ref, w_ref, x_ref, poly_ref,
    o_ref, send_ref, recv_ref, extra_out, extra_in, rows_out, rows_in, sums_out, sums_in,
    scale, stage, extra_stage, rows_tmp, rows_stage, poly, own, cross, listed, extra, far_rows, sums, far_sums, result,
    load_sem, stage_sem, send_sem, recv_sem, poly_sem, field_sem, out_sem, extra_sems, rows_sems, sums_sems, *held,
):
    devices, side = layers * grids, grids // 2
    tiles, pitch = lats // SUBLANES, held[0].shape[0] // SUBLANES
    columns = len(held) // tiles
    local_pairs, half, degrees = o_ref.shape
    chunk = 2
    chunks, dropped = local_pairs // chunk, 2 * len(caps)
    full_chunks = (local_pairs - dropped) // chunk
    per_group = SUBLANES // chunk
    tallest = max(caps)
    starts = [2 * sum(caps[:index]) for index in range(len(caps))]
    my_layer, my_grid = lax.axis_index("layer"), lax.axis_index("grid")
    me = my_layer * grids + my_grid
    my_side = my_grid // side
    partner = lax.rem(my_grid + side, grids)
    side_me = my_layer * side + lax.rem(my_grid, side)
    parts, rows = poly.shape[0], poly.shape[1]
    offset = rows - degrees

    def look(kind, grid, index):
        return table_ref[kind * grids + grid, index]

    def loads(column, tile):
        for row in range(SUBLANES):
            yield pltpu.make_async_copy(
                x_ref.at[pl.ds((tile * SUBLANES + row) * waves, waves), pl.ds(column * LANES, LANES)],
                held[column * tiles + tile].at[pl.ds(row * pitch, waves)],
                load_sem.at[column, tile, row],
            )

    def poly_copies(group):
        spots = pl.ds(pl.multiple_of(group * SUBLANES, SUBLANES), SUBLANES)
        for part in range(parts):
            yield pltpu.make_async_copy(
                poly_ref.at[:, spots, pl.ds(part * LANES, LANES)],
                poly.at[part, pl.ds(offset, degrees)],
                poly_sem.at[part],
            )

    far_lanes = pl.ds(pl.multiple_of((2 * my_layer + 1 - my_side) * LANES, LANES), LANES)
    rows_copy = pltpu.make_async_copy(
        poly_ref.at[pl.ds(degrees - tallest, tallest), :, far_lanes], rows_tmp, rows_sems.at[0]
    )
    rows_copy.start()
    for tile in range(tiles):
        for column in range(columns):
            for copy in loads(column, tile):
                copy.start()

    barrier = pltpu.get_barrier_semaphore()

    def greet(step, carry):
        other = lax.rem(me + step, devices)
        pl.semaphore_signal(
            barrier, inc=1, device_id=(other // grids, lax.rem(other, grids)), device_id_type=MESH
        )
        return carry

    lax.fori_loop(1, devices, greet, 0)

    row_ids = lax.broadcasted_iota(jnp.int32, (SUBLANES, LANES), 0)
    for tile in range(tiles):
        value = jnp.zeros((SUBLANES, LANES), jnp.float32)
        for row in range(SUBLANES):
            value = jnp.where(row_ids == row, w_ref[tile * SUBLANES + row], value)
        scale[tile] = value
    for part in range(parts):
        poly[part, pl.ds(0, offset)] = jnp.zeros((offset, SUBLANES, LANES), jnp.float32)
    sums[...] = jnp.zeros(sums.shape, jnp.float32)

    rows_copy.wait()
    flat_rows = rows_tmp.reshape(tallest * local_pairs, LANES)
    for k in range(dropped):
        cap = caps[k // 2]
        spot = look(SPOT, my_grid, k)
        picked = flat_rows[pl.ds((tallest - cap) * local_pairs + spot, cap, stride=local_pairs), :]
        rows_stage[pl.ds(starts[k // 2] + (k % 2) * cap, cap)] = picked
    rows_copy = pltpu.make_async_copy(rows_stage, rows_out, rows_sems.at[0])
    rows_copy.start()
    rows_copy.wait()
    pl.semaphore_wait(barrier, devices - 1)
    rows_send = pltpu.make_async_remote_copy(
        src_ref=rows_out,
        dst_ref=rows_in.at[my_layer],
        send_sem=rows_sems.at[1],
        recv_sem=rows_sems.at[2],
        device_id=(my_layer, partner),
        device_id_type=MESH,
    )
    rows_send.start()

    in_low = lax.broadcasted_iota(jnp.int32, (SUBLANES, LANES), 1) < half

    def gather(count, waves_of, target, first):
        for tile in range(tiles):
            for column in range(columns):
                if first:
                    for copy in loads(column, tile):
                        copy.wait()
                x = held[column * tiles + tile]
                weight = scale[tile]

                def step(q, carry):
                    one_wave, two_wave, grid, place = waves_of(q)
                    one = x[pl.ds(one_wave, SUBLANES, stride=pitch), :] * weight
                    two = x[pl.ds(two_wave, SUBLANES, stride=pitch), :] * weight
                    span = target.shape[0] // layers
                    lower, upper = 2 * column * span + grid, (2 * column + 1) * span + grid
                    spots = pl.ds(tile * SUBLANES, SUBLANES)
                    target[lower, place, spots] = jnp.where(in_low, one, pltpu.roll(two, half, 1))
                    target[upper, place, spots] = jnp.where(in_low, pltpu.roll(one, half, 1), two)
                    return carry

                lax.fori_loop(0, count, step, 0, unroll=8)

    def put(target, out, kept, here):
        one = pltpu.make_async_copy(target, out, stage_sem.at[0])
        two = pltpu.make_async_copy(target.at[here], kept, stage_sem.at[1])
        one.start()
        two.start()
        one.wait()
        two.wait()

    def pack(index, first):
        def waves_of(q):
            grid, place = q // chunk, lax.rem(q, chunk)
            across = grid // side != my_side
            head = place == 0
            a0, a1 = look(SLOT, grid, index * chunk), look(SLOT, grid, index * chunk + 1)
            b0, b1 = look(LISTED, grid, index * chunk), look(LISTED, grid, index * chunk + 1)
            a = jnp.where(head, a0, a1)
            one = jnp.where(across, jnp.where(head, a0, b0), a)
            two = jnp.where(across, jnp.where(head, a1, b1), waves - 1 - a)
            return one, two, grid, place

        gather(grids * chunk, waves_of, stage, first)
        put(stage, send_ref.at[index], recv_ref.at[index, me], me)

    def send(index):
        def step(k, carry):
            other = lax.rem(me + k, devices)
            layer, grid = other // grids, lax.rem(other, grids)
            short = (index >= full_chunks) & (grid // side != my_side)

            def start(count):
                pltpu.make_async_remote_copy(
                    src_ref=send_ref.at[index, other, pl.ds(0, count)],
                    dst_ref=recv_ref.at[index, me, pl.ds(0, count)],
                    send_sem=send_sem.at[index],
                    recv_sem=recv_sem.at[index],
                    device_id=(layer, grid),
                    device_id_type=MESH,
                ).start()

            @pl.when(short)
            def _():
                start(1)

            @pl.when(jnp.logical_not(short))
            def _():
                start(2)

            return carry

        lax.fori_loop(1, devices, step, 0)

    def whole(ref, index, sem):
        @pl.when(index < full_chunks)
        def _():
            block = ref.at[index, pl.ds(0, devices - 1)]
            pltpu.make_async_copy(block, block, sem.at[index]).wait()

        @pl.when(index >= full_chunks)
        def _():
            block = ref.at[index, pl.ds(0, 3 * devices // 4 - 1)]
            pltpu.make_async_copy(block, block, sem.at[index]).wait()

    def extra_wait(ref, sem):
        block = ref.at[pl.ds(0, layers * side - 1)]
        pltpu.make_async_copy(block, block, sem).wait()

    def send_extra():
        def waves_of(q):
            grid, place = q // len(caps), lax.rem(q, len(caps))
            owner = lax.rem((1 - my_side) * side + grid, grids)
            return look(GONE, owner, 2 * place), look(GONE, owner, 2 * place + 1), grid, place

        gather(side * len(caps), waves_of, extra_stage, False)
        put(extra_stage, extra_out, extra_in.at[side_me], side_me)

        def step(k, carry):
            other = lax.rem(side_me + k, layers * side)
            pltpu.make_async_remote_copy(
                src_ref=extra_out.at[other],
                dst_ref=extra_in.at[side_me],
                send_sem=extra_sems.at[0],
                recv_sem=extra_sems.at[1],
                device_id=(other // side, my_side * side + lax.rem(other, side)),
                device_id_type=MESH,
            ).start()
            return carry

        lax.fori_loop(1, layers * side, step, 0)

    def forward():
        rows_send.wait_recv()

        def step(k, carry):
            pltpu.make_async_remote_copy(
                src_ref=rows_in.at[my_layer],
                dst_ref=rows_in.at[my_layer],
                send_sem=rows_sems.at[3],
                recv_sem=rows_sems.at[4],
                device_id=(lax.rem(my_layer + k, layers), my_grid),
                device_id_type=MESH,
            ).start()
            return carry

        lax.fori_loop(1, layers, step, 0)

    def forward_wait(sem):
        block = rows_in.at[pl.ds(0, layers - 1)]
        pltpu.make_async_copy(block, block, sem).wait()

    sums_send = pltpu.make_async_remote_copy(
        src_ref=sums_out,
        dst_ref=sums_in,
        send_sem=sums_sems.at[0],
        recv_sem=sums_sems.at[1],
        device_id=(my_layer, partner),
        device_id_type=MESH,
    )

    def multiply(left, right):
        right = jnp.concatenate(split(right), axis=1)
        high, low = split(left)
        product = jnp.dot(high, right, preferred_element_type=jnp.float32)
        product = product + jnp.dot(low, right, preferred_element_type=jnp.float32)
        return product[:, :LANES] + product[:, LANES:]

    def help_partner():
        extra_wait(extra_in, extra_sems.at[1])
        forward_wait(rows_sems.at[4])
        one = pltpu.make_async_copy(extra_in, extra, field_sem.at[0, 0])
        two = pltpu.make_async_copy(rows_in, far_rows, field_sem.at[1, 0])
        one.start()
        two.start()
        one.wait()
        two.wait()
        for index, cap in enumerate(caps):
            right = extra[:, index].reshape(layers * side * lats, LANES)
            both = []
            for k in range(2):
                spots = pl.ds(starts[index] + k * cap, cap)
                both.append(jnp.concatenate([far_rows[layer, spots] for layer in range(layers)], axis=1))
            both = multiply(jnp.concatenate(both, axis=0), right)
            low = lax.broadcasted_iota(jnp.int32, (cap, LANES), 1) < half
            far_sums[pl.ds(starts[index] // 2, cap)] = jnp.where(low, both[:cap], both[cap:])
        copy = pltpu.make_async_copy(far_sums, sums_out, field_sem.at[0, 0])
        copy.start()
        copy.wait()
        sums_send.start()

    def take_sums():
        sums_send.wait_recv()
        copies = [
            pltpu.make_async_copy(
                sums_in.at[pl.ds(starts[index] // 2, cap)],
                sums.at[index, pl.ds(tallest - cap, cap)],
                sums_sems.at[2 + index],
            )
            for index, cap in enumerate(caps)
        ]
        for copy in copies:
            copy.start()
        for copy in copies:
            copy.wait()

    pack(0, True)
    send(0)
    send_extra()
    for copy in poly_copies(0):
        copy.start()

    def prepare(index, carry):
        pack(index, False)
        send(index)
        return carry

    lax.fori_loop(1, ahead, prepare, 0)

    def arrive(index, carry):
        @pl.when(index + ahead < chunks)
        def _():
            prepare(index + ahead, 0)

        whole(recv_ref, index, recv_sem)
        return carry

    def consume(index, carry):
        group, place = index // per_group, lax.rem(index, per_group)

        @pl.when(place == 0)
        def _():
            for copy in poly_copies(group):
                copy.wait()

        near, far = my_side * side, (1 - my_side) * side
        copies = []
        for layer in range(layers):
            copies.append(
                pltpu.make_async_copy(
                    recv_ref.at[index, pl.ds(layer * grids + near, side)], own.at[layer], field_sem.at[0, layer]
                )
            )
            copies.append(
                pltpu.make_async_copy(
                    recv_ref.at[index, pl.ds(layer * grids + far, side), 0], cross.at[layer], field_sem.at[1, layer]
                )
            )
        lists = [
            pltpu.make_async_copy(
                recv_ref.at[index, pl.ds(layer * grids + far, side), 1], listed.at[index, layer], field_sem.at[2, layer]
            )
            for layer in range(layers)
        ]

        @pl.when(index < full_chunks)
        def _():
            for copy in lists:
                copy.start()

        for copy in copies:
            copy.start()
        for copy in copies:
            copy.wait()

        @pl.when(index < full_chunks)
        def _():
            for copy in lists:
                copy.wait()

        def pair(p, carry):
            q = index * chunk + p
            limit = waves - look(SLOT, my_grid, q)
            block = (layers * side * lats, LANES)
            near_x = own[:, :, pl.ds(p, 1)].reshape(block)
            low = lax.broadcasted_iota(jnp.int32, block, 1) < half
            first = cross[...].reshape(block)
            first = jnp.where(p == 0, first, pltpu.roll(first, half, 1))
            second = listed[pl.ds(look(LIST_TILE, my_grid, q), 1)].reshape(block)
            second = jnp.where(look(LIST_SIDE, my_grid, q) == 1, second, pltpu.roll(second, half, 1))
            keep = look(KEPT, my_grid, q)
            second = jnp.where(keep == 1, second, 0.0)
            right = jnp.concatenate([near_x, jnp.where(low, first, second)], axis=0)
            spots = pl.ds(place * chunk + p, rows, stride=SUBLANES)
            order = [2 * layer + my_side for layer in range(layers)]
            order += [2 * layer + 1 - my_side for layer in range(layers)]
            left = [poly.at[part].reshape(rows * SUBLANES, LANES)[spots, :] for part in order]
            product = multiply(jnp.concatenate(left, axis=1), right)
            more = sums[pl.ds(look(RANK_TILE, my_grid, q), 1)].reshape(tallest, LANES)
            more = jnp.where(look(RANK_SIDE, my_grid, q) == 1, more, pltpu.roll(more, half, 1))
            high = lax.broadcasted_iota(jnp.int32, more.shape, 1) >= half
            more = jnp.where(high & (keep == 0), more, 0.0)
            product = jnp.concatenate([product[: rows - tallest], product[rows - tallest :] + more], axis=0)
            total = product.T
            ids = lax.broadcasted_iota(jnp.int32, (half, rows), 1) - offset
            result[p] = jnp.where(ids < limit, total[:half], total[half:])[:, offset:]
            return carry

        lax.fori_loop(0, chunk, pair, 0)

        @pl.when((place == per_group - 1) & (index + 1 < chunks))
        def _():
            for copy in poly_copies(group + 1):
                copy.start()

        copy = pltpu.make_async_copy(result, o_ref.at[pl.ds(index * chunk, chunk)], out_sem)
        copy.start()
        copy.wait()
        return carry

    def step(index, carry):
        arrive(index, 0)
        return consume(index, 0)

    lax.fori_loop(0, stops[0], arrive, 0)
    forward()
    lax.fori_loop(stops[0], stops[1], arrive, 0)
    help_partner()
    lax.fori_loop(stops[1], stops[2], arrive, 0)
    take_sums()
    lax.fori_loop(0, stops[2], consume, 0)
    lax.fori_loop(stops[2], chunks, step, 0)

    def finish(index, carry):
        whole(send_ref, index, send_sem)
        return carry

    lax.fori_loop(0, chunks, finish, 0)
    rows_send.wait_send()
    sums_send.wait_send()
    forward_wait(rows_sems.at[3])
    extra_wait(extra_out, extra_sems.at[0])


def shared_transform(layers, grids, caps, fourier, weights, legendre, table):
    local_pairs, degrees, all_lats = legendre.shape
    lats, waves, all_fields = fourier.shape
    half = all_fields // layers
    devices, side, count = layers * grids, grids // 2, len(caps)
    chunk = 2
    chunks = local_pairs // chunk
    ahead = min(3, chunks)
    first = max(1, chunks // 8)
    stops = (first, max(first, chunks * 5 // 16), chunks // 2)
    rows = (degrees + SUBLANES - 1) // SUBLANES * SUBLANES
    columns, tiles, pitch = all_fields // LANES, lats // SUBLANES, waves + SUBLANES
    block = (devices, chunk, lats, LANES)
    near = (layers * side, count, lats, LANES)
    tall, height = max(caps), sum(caps)
    hbm = pl.BlockSpec(memory_space=pl.ANY)
    smem = pl.BlockSpec(memory_space=pltpu.SMEM)

    def shape(*sizes):
        return jax.ShapeDtypeStruct(sizes, jnp.float32)

    def vmem(*sizes):
        return pltpu.VMEM(sizes, jnp.float32)

    return pl.pallas_call(
        functools.partial(shared_kernel, layers, grids, waves, lats, caps, ahead, stops),
        in_specs=[smem, smem, hbm, hbm],
        out_specs=[hbm] * 9,
        out_shape=[
            shape(local_pairs, half, degrees),
            shape(chunks, *block),
            shape(chunks, *block),
            shape(*near),
            shape(*near),
            shape(2 * height, LANES),
            shape(layers, 2 * height, LANES),
            shape(height, LANES),
            shape(height, LANES),
        ],
        scratch_shapes=[
            vmem(tiles, SUBLANES, LANES),
            vmem(*block),
            vmem(*near),
            vmem(tall, local_pairs, LANES),
            vmem(2 * height, LANES),
            vmem(all_lats // LANES, rows, SUBLANES, LANES),
            vmem(layers, side, chunk, lats, LANES),
            vmem(layers, side, lats, LANES),
            vmem((local_pairs - 2 * count) // chunk, layers, side, lats, LANES),
            vmem(*near),
            vmem(layers, 2 * height, LANES),
            vmem(count, tall, LANES),
            vmem(height, LANES),
            vmem(chunk, half, degrees),
            pltpu.SemaphoreType.DMA((columns, tiles, SUBLANES)),
            pltpu.SemaphoreType.DMA((2,)),
            pltpu.SemaphoreType.DMA((chunks,)),
            pltpu.SemaphoreType.DMA((chunks,)),
            pltpu.SemaphoreType.DMA((all_lats // LANES,)),
            pltpu.SemaphoreType.DMA((3, layers)),
            pltpu.SemaphoreType.DMA,
            pltpu.SemaphoreType.DMA((2,)),
            pltpu.SemaphoreType.DMA((5,)),
            pltpu.SemaphoreType.DMA((2 + count,)),
        ]
        + [vmem(SUBLANES * pitch, LANES)] * (columns * tiles),
        compiler_params=pltpu.CompilerParams(
            collective_id=1, has_side_effects=True, vmem_limit_bytes=63 * 2**20
        ),
        name="shared",
    )(table, weights, fourier.reshape(lats * waves, all_fields), legendre.transpose(1, 0, 2))[0]


def row_caps(pairs, local_pairs):
    caps = []
    for k in range(2, local_pairs // 4 + 1, 2):
        share = k / (local_pairs + 1)
        spread = (pairs + 1) * (share * (1 - share) / (local_pairs + 2)) ** 0.5
        caps.append(int((pairs + 1) * share + 3.25 * spread + 7) // 8 * 8)
    return tuple(caps)


def transform(layers, grids, fourier, weights, legendre, pair_slots):
    local_pairs, degrees, all_lats = legendre.shape
    waves = 2 * pair_slots.shape[0]
    lats, _, all_fields = fourier.shape
    half = all_fields // layers
    devices = layers * grids
    chunk = 2
    chunks = local_pairs // chunk
    ahead = min(3, chunks)
    rows = (degrees + SUBLANES - 1) // SUBLANES * SUBLANES
    columns, tiles, pitch = all_fields // LANES, lats // SUBLANES, waves + SUBLANES
    block = (devices, chunk, lats, LANES)
    hbm = pl.BlockSpec(memory_space=pl.ANY)
    smem = pl.BlockSpec(memory_space=pltpu.SMEM)
    return pl.pallas_call(
        functools.partial(transform_kernel, layers, grids, waves, lats, chunk, ahead),
        in_specs=[smem, smem, hbm, hbm],
        out_specs=[hbm, hbm, hbm],
        out_shape=[
            jax.ShapeDtypeStruct((local_pairs, half, degrees), jnp.float32),
            jax.ShapeDtypeStruct((chunks,) + block, jnp.float32),
            jax.ShapeDtypeStruct((chunks,) + block, jnp.float32),
        ],
        scratch_shapes=[
            pltpu.VMEM((tiles, SUBLANES, LANES), jnp.float32),
            pltpu.VMEM(block, jnp.float32),
            pltpu.VMEM((all_lats // LANES, rows, SUBLANES, LANES), jnp.float32),
            pltpu.VMEM(block, jnp.float32),
            pltpu.VMEM((chunk, half, degrees), jnp.float32),
            pltpu.SemaphoreType.DMA((columns, tiles, SUBLANES)),
            pltpu.SemaphoreType.DMA((2,)),
            pltpu.SemaphoreType.DMA((chunks,)),
            pltpu.SemaphoreType.DMA((chunks,)),
            pltpu.SemaphoreType.DMA((all_lats // LANES,)),
            pltpu.SemaphoreType.DMA,
            pltpu.SemaphoreType.DMA,
        ]
        + [pltpu.VMEM((SUBLANES * pitch, LANES), jnp.float32)] * (columns * tiles),
        compiler_params=pltpu.CompilerParams(
            collective_id=0, has_side_effects=True, vmem_limit_bytes=60 * 2**20
        ),
        name="transform",
    )(pair_slots, weights, fourier.reshape(lats * waves, all_fields), legendre.transpose(1, 0, 2))[0]


def shards(layers, grids, fourier, weights, legendre, pair_slots):
    pairs, local_pairs = pair_slots.shape[0], legendre.shape[0]
    caps = row_caps(pairs, local_pairs)
    table, fits = plan(pair_slots, grids, 2 * pairs, caps)
    out = lax.cond(
        fits[0] == 1,
        lambda: shared_transform(layers, grids, caps, fourier, weights, legendre, table),
        lambda: transform(layers, grids, fourier, weights, legendre, pair_slots),
    )
    return out.transpose(0, 2, 1)


def solution(mesh):
    in_specs = (P(("layer", "grid"), None, None), P(("layer", "grid")), P("grid", None, None), P())
    out_specs = P("grid", None, "layer")
    body = functools.partial(shards, mesh.shape["layer"], mesh.shape["grid"])
    return jax.shard_map(body, mesh=mesh, in_specs=in_specs, out_specs=out_specs, check_vma=False)
```

```python
import functools

import jax
import jax.numpy as jnp
from jax import lax
from jax.experimental import pallas as pl
from jax.experimental.pallas import tpu as pltpu
from jax.sharding import PartitionSpec as P

LANES = 128
SUBLANES = 8
MESH = pl.DeviceIdType.MESH


def split(x):
    high = x.astype(jnp.bfloat16)
    return high, (x - high.astype(jnp.float32)).astype(jnp.bfloat16)


def transform_kernel(
    layers, grids, waves, lats, chunk, ahead,
    slots_ref, w_ref, x_ref, poly_ref,
    o_ref, send_ref, recv_ref,
    scale, stage, poly, fields, result,
    load_sem, stage_sem, send_sem, recv_sem, poly_sem, field_sem, out_sem, *held,
):
    devices = layers * grids
    tiles, pitch = lats // SUBLANES, held[0].shape[0] // SUBLANES
    columns = len(held) // tiles
    local_pairs, half, degrees = o_ref.shape
    chunks = local_pairs // chunk
    per_group = SUBLANES // chunk
    my_layer, my_grid = lax.axis_index("layer"), lax.axis_index("grid")
    me = my_layer * grids + my_grid

    def loads(column, tile):
        for row in range(SUBLANES):
            yield pltpu.make_async_copy(
                x_ref.at[pl.ds((tile * SUBLANES + row) * waves, waves), pl.ds(column * LANES, LANES)],
                held[column * tiles + tile].at[pl.ds(row * pitch, waves)],
                load_sem.at[column, tile, row],
            )

    def poly_copies(group):
        rows = pl.ds(pl.multiple_of(group * SUBLANES, SUBLANES), SUBLANES)
        for part in range(poly.shape[0]):
            yield pltpu.make_async_copy(
                poly_ref.at[:, rows, pl.ds(part * LANES, LANES)],
                poly.at[part, pl.ds(0, degrees)],
                poly_sem.at[part],
            )

    def whole(ref, index, sem):
        block = ref.at[index, pl.ds(0, devices - 1)]
        return pltpu.make_async_copy(block, block, sem.at[index])

    for tile in range(tiles):
        for column in range(columns):
            for copy in loads(column, tile):
                copy.start()

    barrier = pltpu.get_barrier_semaphore()

    def greet(step, carry):
        other = lax.rem(me + step, devices)
        pl.semaphore_signal(
            barrier, inc=1, device_id=(other // grids, lax.rem(other, grids)), device_id_type=MESH
        )
        return carry

    lax.fori_loop(1, devices, greet, 0)

    row_ids = lax.broadcasted_iota(jnp.int32, (SUBLANES, LANES), 0)
    for tile in range(tiles):
        value = jnp.zeros((SUBLANES, LANES), jnp.float32)
        for row in range(SUBLANES):
            value = jnp.where(row_ids == row, w_ref[tile * SUBLANES + row], value)
        scale[tile] = value
    parts, rows = poly.shape[0], poly.shape[1]
    for part in range(parts):
        poly[part, pl.ds(degrees, rows - degrees)] = jnp.zeros((rows - degrees, SUBLANES, LANES), jnp.float32)

    in_low = lax.broadcasted_iota(jnp.int32, (SUBLANES, LANES), 1) < half

    def pack(index, first):
        for tile in range(tiles):
            for column in range(columns):
                if first:
                    for copy in loads(column, tile):
                        copy.wait()
                x = held[column * tiles + tile]
                weight = scale[tile]

                def step(q, carry):
                    grid, place = q // chunk, lax.rem(q, chunk)
                    a = slots_ref[grid * local_pairs + index * chunk + place]
                    one = x[pl.ds(a, SUBLANES, stride=pitch), :] * weight
                    two = x[pl.ds(waves - 1 - a, SUBLANES, stride=pitch), :] * weight
                    lower, upper = 2 * column * grids + grid, (2 * column + 1) * grids + grid
                    rows = pl.ds(tile * SUBLANES, SUBLANES)
                    stage[lower, place, rows] = jnp.where(in_low, one, pltpu.roll(two, half, 1))
                    stage[upper, place, rows] = jnp.where(in_low, pltpu.roll(one, half, 1), two)
                    return carry

                lax.fori_loop(0, grids * chunk, step, 0, unroll=8)
        out = pltpu.make_async_copy(stage, send_ref.at[index], stage_sem.at[0])
        own = pltpu.make_async_copy(stage.at[me], recv_ref.at[index, me], stage_sem.at[1])
        out.start()
        own.start()
        out.wait()
        own.wait()

    def send(index):
        def step(k, carry):
            other = lax.rem(me + k, devices)
            pltpu.make_async_remote_copy(
                src_ref=send_ref.at[index, other],
                dst_ref=recv_ref.at[index, me],
                send_sem=send_sem.at[index],
                recv_sem=recv_sem.at[index],
                device_id=(other // grids, lax.rem(other, grids)),
                device_id_type=MESH,
            ).start()
            return carry

        lax.fori_loop(1, devices, step, 0)

    pack(0, True)
    pl.semaphore_wait(barrier, devices - 1)
    send(0)
    for copy in poly_copies(0):
        copy.start()

    def prepare(index, carry):
        pack(index, False)
        send(index)
        return carry

    lax.fori_loop(1, ahead, prepare, 0)

    def consume(index, carry):
        @pl.when(index + ahead < chunks)
        def _():
            prepare(index + ahead, 0)

        group, place = index // per_group, lax.rem(index, per_group)

        @pl.when(place == 0)
        def _():
            for copy in poly_copies(group):
                copy.wait()

        whole(recv_ref, index, recv_sem).wait()
        copy = pltpu.make_async_copy(recv_ref.at[index], fields, field_sem)
        copy.start()
        copy.wait()

        def pair(p, carry):
            limit = waves - slots_ref[my_grid * local_pairs + index * chunk + p]
            x = fields[:, pl.ds(p, 1)].reshape(devices * lats, LANES)
            right = jnp.concatenate(split(x), axis=1)
            spots = pl.ds(place * chunk + p, rows, stride=SUBLANES)
            left = [poly.at[part].reshape(rows * SUBLANES, LANES)[spots, :] for part in range(parts)]
            high, low = split(jnp.concatenate(left, axis=1))
            product = jnp.dot(high, right, preferred_element_type=jnp.float32)
            product = product + jnp.dot(low, right, preferred_element_type=jnp.float32)
            total = (product[:, :LANES] + product[:, LANES:]).T
            ids = lax.broadcasted_iota(jnp.int32, (half, rows), 1)
            result[p] = jnp.where(ids < limit, total[:half], total[half:])[:, :degrees]
            return carry

        lax.fori_loop(0, chunk, pair, 0)

        @pl.when((place == per_group - 1) & (index + 1 < chunks))
        def _():
            for copy in poly_copies(group + 1):
                copy.start()

        copy = pltpu.make_async_copy(result, o_ref.at[pl.ds(index * chunk, chunk)], out_sem)
        copy.start()
        copy.wait()
        return carry

    lax.fori_loop(0, chunks, consume, 0)

    def finish(index, carry):
        whole(send_ref, index, send_sem).wait()
        return carry

    lax.fori_loop(0, chunks, finish, 0)

def plan_kernel(grids, dropped, most, tallest, slots_ref, table_ref, index_ref, flag_ref):
    pairs = slots_ref.shape[0]
    waves, local_pairs = 2 * pairs, table_ref.shape[1]
    shape = (grids, local_pairs)
    lane = lax.broadcasted_iota(jnp.int32, shape, 1)
    code = lax.broadcasted_iota(jnp.int32, shape, 0) * local_pairs + lane
    zero = jnp.zeros(shape, jnp.int32)
    a = zero
    for p in range(pairs):
        a = jnp.where(code == p, slots_ref[p], a)
    b = waves - 1 - a
    rank = zero
    for p in range(local_pairs):
        rank = rank + jnp.where(a[:, p : p + 1] < a, 1, 0)
    kept = jnp.where(rank < dropped, 0, 1)
    place = zero
    for p in range(local_pairs):
        place = place + jnp.where(lane > p, kept[:, p : p + 1], 0)
    listed, gone, spot = zero, zero, zero
    for p in range(local_pairs):
        wave = b[:, p : p + 1]
        listed = listed + jnp.where((lane == place[:, p : p + 1]) & (kept[:, p : p + 1] == 1), wave, 0)
        mine = (lane == rank[:, p : p + 1]) & (lane < dropped)
        gone = gone + jnp.where(mine, wave, 0)
        spot = spot + jnp.where(mine, p, 0)
    count = jnp.where(lane < dropped, waves - gone, 0)
    end = zero
    for k in range(dropped):
        end = end + jnp.where(lane >= k, count[:, k : k + 1], 0)
    begin = end - count
    over = jnp.where((end > most) | (count > tallest), 1.0, 0.0)
    flag_ref[0] = (jnp.sum(over) < 0.5).astype(jnp.int32)
    place = jnp.where(kept == 1, place, 0)
    rank = jnp.where(kept == 1, 0, rank)
    bound = zero
    for k in range(dropped):
        bound = bound + jnp.where(rank == k, end[:, k : k + 1], 0)
    kinds = (a, listed, gone, place // 2, lax.rem(place, 2), kept, begin, end, bound)
    for index, value in enumerate(kinds):
        table_ref[pl.ds(index * grids, grids)] = value
    me = lax.axis_index("grid")

    def mine(value):
        row = jnp.zeros((1, local_pairs), jnp.int32)
        for grid in range(grids):
            row = row + jnp.where(grid == me, value[grid : grid + 1], 0)
        return row

    my_begin, my_end, my_spot = mine(begin), mine(end), mine(spot)
    slot = lax.broadcasted_iota(jnp.int32, index_ref.shape, 0) * LANES
    slot = slot + lax.broadcasted_iota(jnp.int32, index_ref.shape, 1)
    row = jnp.zeros(index_ref.shape, jnp.int32)
    for k in range(dropped):
        start, stop, place = my_begin[:, k : k + 1], my_end[:, k : k + 1], my_spot[:, k : k + 1]
        inside = (slot >= start) & (slot < stop)
        row = jnp.where(inside, (tallest - stop + slot) * local_pairs + place, row)
    index_ref[...] = jnp.maximum(row, 0)


KINDS = 9
SLOT, LISTED, GONE, LIST_TILE, LIST_SIDE, KEPT, BEGIN, END, BOUND = range(KINDS)


def plan(pair_slots, grids, dropped, most, tallest):
    return pl.pallas_call(
        functools.partial(plan_kernel, grids, dropped, most, tallest),
        in_specs=[pl.BlockSpec(memory_space=pltpu.SMEM)],
        out_specs=[pl.BlockSpec(memory_space=pltpu.VMEM)] * 2 + [pl.BlockSpec(memory_space=pltpu.SMEM)],
        out_shape=[
            jax.ShapeDtypeStruct((KINDS * grids, pair_slots.shape[0] // grids), jnp.int32),
            jax.ShapeDtypeStruct((pl.cdiv(most, LANES), LANES), jnp.int32),
            jax.ShapeDtypeStruct((1,), jnp.int32),
        ],
        name="plan",
    )(pair_slots)


def shared_kernel(
    layers, grids, waves, lats, dropped, tallest, ahead, help_at, wait_end,
    table_ref, index_ref, w_ref, x_ref, poly_ref,
    o_ref, send_ref, recv_ref, extra_out, extra_in, rows_out, rows_in, sums_out, sums_in,
    scale, stage, extra_stage, rows_tmp, rows_stage, poly, own, cross, listed, extra, far_rows, taken, sums, gathered, far_sums, result,
    load_sem, stage_sem, send_sem, recv_sem, poly_sem, field_sem, out_sem, extra_sems, rows_sems, sums_sems, *held,
):
    devices, side = layers * grids, grids // 2
    tiles, pitch = lats // SUBLANES, held[0].shape[0] // SUBLANES
    columns = len(held) // tiles
    local_pairs, half, degrees = o_ref.shape
    chunk = 2
    chunks = local_pairs // chunk
    full_chunks = (local_pairs - dropped) // chunk
    per_group = SUBLANES // chunk
    most = rows_out.shape[0]
    my_layer, my_grid = lax.axis_index("layer"), lax.axis_index("grid")
    me = my_layer * grids + my_grid
    my_side = my_grid // side
    partner = lax.rem(my_grid + side, grids)
    side_me = my_layer * side + lax.rem(my_grid, side)
    parts, rows = poly.shape[0], poly.shape[1]
    offset = rows - degrees

    def look(kind, grid, index):
        return table_ref[kind * grids + grid, index]

    def loads(column, tile):
        for row in range(SUBLANES):
            yield pltpu.make_async_copy(
                x_ref.at[pl.ds((tile * SUBLANES + row) * waves, waves), pl.ds(column * LANES, LANES)],
                held[column * tiles + tile].at[pl.ds(row * pitch, waves)],
                load_sem.at[column, tile, row],
            )

    def poly_copies(group):
        spots = pl.ds(pl.multiple_of(group * SUBLANES, SUBLANES), SUBLANES)
        for part in range(parts):
            yield pltpu.make_async_copy(
                poly_ref.at[:, spots, pl.ds(part * LANES, LANES)],
                poly.at[part, pl.ds(offset, degrees)],
                poly_sem.at[part],
            )

    far_lanes = pl.ds(pl.multiple_of((2 * my_layer + 1 - my_side) * LANES, LANES), LANES)
    rows_copy = pltpu.make_async_copy(
        poly_ref.at[pl.ds(degrees - tallest, tallest), :, far_lanes], rows_tmp, rows_sems.at[0]
    )
    rows_copy.start()
    for tile in range(tiles):
        for column in range(columns):
            for copy in loads(column, tile):
                copy.start()

    barrier = pltpu.get_barrier_semaphore()

    def greet(step, carry):
        other = lax.rem(me + step, devices)
        pl.semaphore_signal(
            barrier, inc=1, device_id=(other // grids, lax.rem(other, grids)), device_id_type=MESH
        )
        return carry

    lax.fori_loop(1, devices, greet, 0)

    row_ids = lax.broadcasted_iota(jnp.int32, (SUBLANES, LANES), 0)
    for tile in range(tiles):
        value = jnp.zeros((SUBLANES, LANES), jnp.float32)
        for row in range(SUBLANES):
            value = jnp.where(row_ids == row, w_ref[tile * SUBLANES + row], value)
        scale[tile] = value
    for part in range(parts):
        poly[part, pl.ds(0, offset)] = jnp.zeros((offset, SUBLANES, LANES), jnp.float32)
    sums[pl.ds(0, tallest)] = jnp.zeros((tallest, LANES), jnp.float32)

    rows_copy.wait()
    flat_rows = rows_tmp.reshape(tallest * local_pairs, LANES)

    def pick(t, carry):
        row = index_ref[t // LANES, lax.rem(t, LANES)]
        rows_stage[pl.ds(t, 1)] = flat_rows[pl.ds(row, 1), :]
        return carry

    lax.fori_loop(0, most, pick, 0, unroll=16)
    rows_copy = pltpu.make_async_copy(rows_stage, rows_out, rows_sems.at[0])
    rows_copy.start()
    rows_copy.wait()
    pl.semaphore_wait(barrier, devices - 1)
    rows_send = pltpu.make_async_remote_copy(
        src_ref=rows_out,
        dst_ref=rows_in.at[my_layer],
        send_sem=rows_sems.at[1],
        recv_sem=rows_sems.at[2],
        device_id=(my_layer, partner),
        device_id_type=MESH,
    )
    rows_send.start()

    in_low = lax.broadcasted_iota(jnp.int32, (SUBLANES, LANES), 1) < half

    def gather(count, waves_of, target, first):
        for tile in range(tiles):
            for column in range(columns):
                if first:
                    for copy in loads(column, tile):
                        copy.wait()
                x = held[column * tiles + tile]
                weight = scale[tile]

                def step(q, carry):
                    one_wave, two_wave, grid, place = waves_of(q)
                    one = x[pl.ds(one_wave, SUBLANES, stride=pitch), :] * weight
                    two = x[pl.ds(two_wave, SUBLANES, stride=pitch), :] * weight
                    span = target.shape[0] // layers
                    lower, upper = 2 * column * span + grid, (2 * column + 1) * span + grid
                    spots = pl.ds(tile * SUBLANES, SUBLANES)
                    target[lower, place, spots] = jnp.where(in_low, one, pltpu.roll(two, half, 1))
                    target[upper, place, spots] = jnp.where(in_low, pltpu.roll(one, half, 1), two)
                    return carry

                lax.fori_loop(0, count, step, 0, unroll=8)

    def put(target, out, kept, here):
        one = pltpu.make_async_copy(target, out, stage_sem.at[0])
        two = pltpu.make_async_copy(target.at[here], kept, stage_sem.at[1])
        one.start()
        two.start()
        one.wait()
        two.wait()

    def pack(index, first):
        def waves_of(q):
            grid, place = q // chunk, lax.rem(q, chunk)
            across = grid // side != my_side
            head = place == 0
            a0, a1 = look(SLOT, grid, index * chunk), look(SLOT, grid, index * chunk + 1)
            b0, b1 = look(LISTED, grid, index * chunk), look(LISTED, grid, index * chunk + 1)
            a = jnp.where(head, a0, a1)
            one = jnp.where(across, jnp.where(head, a0, b0), a)
            two = jnp.where(across, jnp.where(head, a1, b1), waves - 1 - a)
            return one, two, grid, place

        gather(grids * chunk, waves_of, stage, first)
        put(stage, send_ref.at[index], recv_ref.at[index, me], me)

    def send(index):
        def start(k, which, count):
            place = lax.rem(side_me + k, layers * side)
            layer, grid = place // side, which * side + lax.rem(place, side)
            pltpu.make_async_remote_copy(
                src_ref=send_ref.at[index, layer * grids + grid, pl.ds(0, count)],
                dst_ref=recv_ref.at[index, me, pl.ds(0, count)],
                send_sem=send_sem.at[index],
                recv_sem=recv_sem.at[index],
                device_id=(layer, grid),
                device_id_type=MESH,
            ).start()

        def far(k, carry):
            @pl.when(index < full_chunks)
            def _():
                start(k, 1 - my_side, 2)

            @pl.when(index >= full_chunks)
            def _():
                start(k, 1 - my_side, 1)

            return carry

        def near(k, carry):
            start(k, my_side, 2)
            return carry

        lax.fori_loop(0, layers * side, far, 0)
        lax.fori_loop(1, layers * side, near, 0)

    def whole(ref, index, sem):
        @pl.when(index < full_chunks)
        def _():
            block = ref.at[index, pl.ds(0, devices - 1)]
            pltpu.make_async_copy(block, block, sem.at[index]).wait()

        @pl.when(index >= full_chunks)
        def _():
            block = ref.at[index, pl.ds(0, 3 * devices // 4 - 1)]
            pltpu.make_async_copy(block, block, sem.at[index]).wait()

    def extra_wait(ref, sem):
        block = ref.at[pl.ds(0, layers * side - 1)]
        pltpu.make_async_copy(block, block, sem).wait()

    def send_extra():
        def waves_of(q):
            grid, place = q // (dropped // 2), lax.rem(q, dropped // 2)
            owner = lax.rem((1 - my_side) * side + grid, grids)
            return look(GONE, owner, 2 * place), look(GONE, owner, 2 * place + 1), grid, place

        gather(side * dropped // 2, waves_of, extra_stage, False)
        put(extra_stage, extra_out, extra_in.at[side_me], side_me)

        def step(k, carry):
            other = lax.rem(side_me + k, layers * side)
            pltpu.make_async_remote_copy(
                src_ref=extra_out.at[other],
                dst_ref=extra_in.at[side_me],
                send_sem=extra_sems.at[0],
                recv_sem=extra_sems.at[1],
                device_id=(other // side, my_side * side + lax.rem(other, side)),
                device_id_type=MESH,
            ).start()
            return carry

        lax.fori_loop(1, layers * side, step, 0)

    def forward():
        rows_send.wait_recv()

        def step(k, carry):
            pltpu.make_async_remote_copy(
                src_ref=rows_in.at[my_layer],
                dst_ref=rows_in.at[my_layer],
                send_sem=rows_sems.at[3],
                recv_sem=rows_sems.at[4],
                device_id=(lax.rem(my_layer + k, layers), my_grid),
                device_id_type=MESH,
            ).start()
            return carry

        lax.fori_loop(1, layers, step, 0)

    def forward_wait(sem):
        block = rows_in.at[pl.ds(0, layers - 1)]
        pltpu.make_async_copy(block, block, sem).wait()

    sums_send = pltpu.make_async_remote_copy(
        src_ref=sums_out,
        dst_ref=sums_in,
        send_sem=sums_sems.at[0],
        recv_sem=sums_sems.at[1],
        device_id=(my_layer, partner),
        device_id_type=MESH,
    )

    def multiply(left, right):
        right = jnp.concatenate(split(right), axis=1)
        high, low = split(left)
        product = jnp.dot(high, right, preferred_element_type=jnp.float32)
        product = product + jnp.dot(low, right, preferred_element_type=jnp.float32)
        return product[:, :LANES] + product[:, LANES:]

    def help_partner():
        extra_wait(extra_in, extra_sems.at[1])
        forward_wait(rows_sems.at[4])
        one = pltpu.make_async_copy(extra_in, extra, field_sem.at[0, 0])
        two = pltpu.make_async_copy(rows_in, far_rows, field_sem.at[1, 0])
        one.start()
        two.start()
        one.wait()
        two.wait()
        gathered[...] = jnp.zeros(gathered.shape, jnp.float32)
        ids = lax.broadcasted_iota(jnp.int32, (most, LANES), 0)
        low = lax.broadcasted_iota(jnp.int32, (most, LANES), 1) < half

        def tile(index, carry):
            right = extra[:, pl.ds(index, 1)].reshape(layers * side * lats, LANES)
            left = jnp.concatenate([far_rows[layer] for layer in range(layers)], axis=1)
            first, last = look(BEGIN, partner, 2 * index), look(END, partner, 2 * index)
            limit = look(END, partner, 2 * index + 1)
            start = jnp.where(low, first, last)
            stop = jnp.where(low, last, limit)
            gathered[...] += jnp.where((ids >= start) & (ids < stop), multiply(left, right), 0.0)
            return carry

        lax.fori_loop(0, dropped // 2, tile, 0)
        value = gathered[...]
        value = value + pltpu.roll(value, half, 1)
        low = lax.broadcasted_iota(jnp.int32, (most // 2, LANES), 1) < half
        far_sums[...] = jnp.where(low, value[: most // 2], value[most // 2 :])
        copy = pltpu.make_async_copy(far_sums, sums_out, field_sem.at[0, 0])
        copy.start()
        copy.wait()
        sums_send.start()

    def take_sums():
        sums_send.wait_recv()
        copy = pltpu.make_async_copy(sums_in, taken, sums_sems.at[2])
        copy.start()
        copy.wait()
        value = taken[...]
        sums[pl.ds(tallest, most // 2)] = pltpu.roll(value, half, 1)
        sums[pl.ds(tallest + most // 2, most // 2)] = value

    pack(0, True)
    send(0)
    send_extra()
    for copy in poly_copies(0):
        copy.start()
    forward()

    def prepare(index, carry):
        pack(index, False)
        send(index)
        return carry

    lax.fori_loop(1, ahead, prepare, 0)

    def arrive(index, carry):
        @pl.when(index + ahead < chunks)
        def _():
            prepare(index + ahead, 0)

        whole(recv_ref, index, recv_sem)
        return carry

    def consume(index, carry):
        group, place = index // per_group, lax.rem(index, per_group)

        @pl.when(place == 0)
        def _():
            for copy in poly_copies(group):
                copy.wait()

        near, far = my_side * side, (1 - my_side) * side
        copies = []
        for layer in range(layers):
            copies.append(
                pltpu.make_async_copy(
                    recv_ref.at[index, pl.ds(layer * grids + near, side)], own.at[layer], field_sem.at[0, layer]
                )
            )
            copies.append(
                pltpu.make_async_copy(
                    recv_ref.at[index, pl.ds(layer * grids + far, side), 0], cross.at[layer], field_sem.at[1, layer]
                )
            )
        lists = [
            pltpu.make_async_copy(
                recv_ref.at[index, pl.ds(layer * grids + far, side), 1], listed.at[index, layer], field_sem.at[2, layer]
            )
            for layer in range(layers)
        ]

        @pl.when(index < full_chunks)
        def _():
            for copy in lists:
                copy.start()

        for copy in copies:
            copy.start()
        for copy in copies:
            copy.wait()

        @pl.when(index < full_chunks)
        def _():
            for copy in lists:
                copy.wait()

        def pair(p, carry):
            q = index * chunk + p
            limit = waves - look(SLOT, my_grid, q)
            block = (layers * side * lats, LANES)
            near_x = own[:, :, pl.ds(p, 1)].reshape(block)
            low = lax.broadcasted_iota(jnp.int32, block, 1) < half
            first = cross[...].reshape(block)
            first = jnp.where(p == 0, first, pltpu.roll(first, half, 1))
            second = listed[pl.ds(look(LIST_TILE, my_grid, q), 1)].reshape(block)
            second = jnp.where(look(LIST_SIDE, my_grid, q) == 1, second, pltpu.roll(second, half, 1))
            keep = look(KEPT, my_grid, q)
            second = jnp.where(keep == 1, second, 0.0)
            right = jnp.concatenate([near_x, jnp.where(low, first, second)], axis=0)
            spots = pl.ds(place * chunk + p, rows, stride=SUBLANES)
            order = [2 * layer + my_side for layer in range(layers)]
            order += [2 * layer + 1 - my_side for layer in range(layers)]
            left = [poly.at[part].reshape(rows * SUBLANES, LANES)[spots, :] for part in order]
            product = multiply(jnp.concatenate(left, axis=1), right)
            more = sums[pl.ds(look(BOUND, my_grid, q), tallest), :]
            high = lax.broadcasted_iota(jnp.int32, more.shape, 1) >= half
            more = jnp.where(high & (keep == 0), more, 0.0)
            product = jnp.concatenate([product[: rows - tallest], product[rows - tallest :] + more], axis=0)
            total = product.T
            ids = lax.broadcasted_iota(jnp.int32, (half, rows), 1) - offset
            result[p] = jnp.where(ids < limit, total[:half], total[half:])[:, offset:]
            return carry

        lax.fori_loop(0, chunk, pair, 0, unroll=True)

        @pl.when((place == per_group - 1) & (index + 1 < chunks))
        def _():
            for copy in poly_copies(group + 1):
                copy.start()

        copy = pltpu.make_async_copy(result, o_ref.at[pl.ds(index * chunk, chunk)], out_sem)
        copy.start()
        copy.wait()
        return carry

    def step(index, carry):
        arrive(index, 0)
        late = index - wait_end
        begin = jnp.where(late < wait_end, 2 * late, index)
        end = jnp.where(late < wait_end, 2 * late + 2, index + 1)
        return lax.fori_loop(begin, end, consume, 0)

    lax.fori_loop(0, help_at, arrive, 0)
    help_partner()
    lax.fori_loop(help_at, wait_end, arrive, 0)
    take_sums()
    lax.fori_loop(wait_end, chunks, step, 0)

    def finish(index, carry):
        whole(send_ref, index, send_sem)
        return carry

    lax.fori_loop(0, chunks, finish, 0)
    rows_send.wait_send()
    sums_send.wait_send()
    forward_wait(rows_sems.at[3])
    extra_wait(extra_out, extra_sems.at[0])


def shared_transform(layers, grids, dropped, most, tallest, fourier, weights, legendre, table, index):
    local_pairs, degrees, all_lats = legendre.shape
    lats, waves, all_fields = fourier.shape
    half = all_fields // layers
    devices, side, count = layers * grids, grids // 2, dropped // 2
    chunk = 2
    chunks = local_pairs // chunk
    ahead = min(3, chunks)
    help_at, wait_end = max(1, chunks // 8), max(1, chunks * 3 // 8)
    rows = (degrees + SUBLANES - 1) // SUBLANES * SUBLANES
    columns, tiles, pitch = all_fields // LANES, lats // SUBLANES, waves + SUBLANES
    block = (devices, chunk, lats, LANES)
    near = (layers * side, count, lats, LANES)
    hbm = pl.BlockSpec(memory_space=pl.ANY)
    smem = pl.BlockSpec(memory_space=pltpu.SMEM)

    def shape(*sizes):
        return jax.ShapeDtypeStruct(sizes, jnp.float32)

    def vmem(*sizes):
        return pltpu.VMEM(sizes, jnp.float32)

    return pl.pallas_call(
        functools.partial(shared_kernel, layers, grids, waves, lats, dropped, tallest, ahead, help_at, wait_end),
        in_specs=[smem, smem, smem, hbm, hbm],
        out_specs=[hbm] * 9,
        out_shape=[
            shape(local_pairs, half, degrees),
            shape(chunks, *block),
            shape(chunks, *block),
            shape(*near),
            shape(*near),
            shape(most, LANES),
            shape(layers, most, LANES),
            shape(most // 2, LANES),
            shape(most // 2, LANES),
        ],
        scratch_shapes=[
            vmem(tiles, SUBLANES, LANES),
            vmem(*block),
            vmem(*near),
            vmem(tallest, local_pairs, LANES),
            vmem(most, LANES),
            vmem(all_lats // LANES, rows, SUBLANES, LANES),
            vmem(layers, side, chunk, lats, LANES),
            vmem(layers, side, lats, LANES),
            vmem((local_pairs - dropped) // chunk, layers, side, lats, LANES),
            vmem(*near),
            vmem(layers, most, LANES),
            vmem(most // 2, LANES),
            vmem(tallest + most, LANES),
            vmem(most, LANES),
            vmem(most // 2, LANES),
            vmem(chunk, half, degrees),
            pltpu.SemaphoreType.DMA((columns, tiles, SUBLANES)),
            pltpu.SemaphoreType.DMA((2,)),
            pltpu.SemaphoreType.DMA((chunks,)),
            pltpu.SemaphoreType.DMA((chunks,)),
            pltpu.SemaphoreType.DMA((all_lats // LANES,)),
            pltpu.SemaphoreType.DMA((3, layers)),
            pltpu.SemaphoreType.DMA,
            pltpu.SemaphoreType.DMA((2,)),
            pltpu.SemaphoreType.DMA((5,)),
            pltpu.SemaphoreType.DMA((3,)),
        ]
        + [vmem(SUBLANES * pitch, LANES)] * (columns * tiles),
        compiler_params=pltpu.CompilerParams(
            collective_id=1, has_side_effects=True, vmem_limit_bytes=63 * 2**20
        ),
        name="shared",
    )(table, index, weights, fourier.reshape(lats * waves, all_fields), legendre.transpose(1, 0, 2))[0]


def row_limits(pairs, local_pairs):
    dropped = max(2, local_pairs * 3 // 8 // 2 * 2)
    shares = [k / (local_pairs + 1) for k in range(1, dropped + 1)]
    means = [(pairs + 1) * share for share in shares]
    spreads = [(pairs + 1) * (share * (1 - share) / (local_pairs + 2)) ** 0.5 for share in shares]
    most = int(sum(means) + 2.6 * sum(spreads) + 15) // 16 * 16
    tallest = int(means[-1] + 3.1 * spreads[-1] + 7) // 8 * 8
    return dropped, most, min(tallest, pairs)


def transform(layers, grids, fourier, weights, legendre, pair_slots):
    local_pairs, degrees, all_lats = legendre.shape
    waves = 2 * pair_slots.shape[0]
    lats, _, all_fields = fourier.shape
    half = all_fields // layers
    devices = layers * grids
    chunk = 2
    chunks = local_pairs // chunk
    ahead = min(3, chunks)
    rows = (degrees + SUBLANES - 1) // SUBLANES * SUBLANES
    columns, tiles, pitch = all_fields // LANES, lats // SUBLANES, waves + SUBLANES
    block = (devices, chunk, lats, LANES)
    hbm = pl.BlockSpec(memory_space=pl.ANY)
    smem = pl.BlockSpec(memory_space=pltpu.SMEM)
    return pl.pallas_call(
        functools.partial(transform_kernel, layers, grids, waves, lats, chunk, ahead),
        in_specs=[smem, smem, hbm, hbm],
        out_specs=[hbm, hbm, hbm],
        out_shape=[
            jax.ShapeDtypeStruct((local_pairs, half, degrees), jnp.float32),
            jax.ShapeDtypeStruct((chunks,) + block, jnp.float32),
            jax.ShapeDtypeStruct((chunks,) + block, jnp.float32),
        ],
        scratch_shapes=[
            pltpu.VMEM((tiles, SUBLANES, LANES), jnp.float32),
            pltpu.VMEM(block, jnp.float32),
            pltpu.VMEM((all_lats // LANES, rows, SUBLANES, LANES), jnp.float32),
            pltpu.VMEM(block, jnp.float32),
            pltpu.VMEM((chunk, half, degrees), jnp.float32),
            pltpu.SemaphoreType.DMA((columns, tiles, SUBLANES)),
            pltpu.SemaphoreType.DMA((2,)),
            pltpu.SemaphoreType.DMA((chunks,)),
            pltpu.SemaphoreType.DMA((chunks,)),
            pltpu.SemaphoreType.DMA((all_lats // LANES,)),
            pltpu.SemaphoreType.DMA,
            pltpu.SemaphoreType.DMA,
        ]
        + [pltpu.VMEM((SUBLANES * pitch, LANES), jnp.float32)] * (columns * tiles),
        compiler_params=pltpu.CompilerParams(
            collective_id=0, has_side_effects=True, vmem_limit_bytes=60 * 2**20
        ),
        name="transform",
    )(pair_slots, weights, fourier.reshape(lats * waves, all_fields), legendre.transpose(1, 0, 2))[0]


def shards(layers, grids, fourier, weights, legendre, pair_slots):
    pairs, local_pairs = pair_slots.shape[0], legendre.shape[0]
    limits = row_limits(pairs, local_pairs)
    table, index, fits = plan(pair_slots, grids, *limits)
    out = lax.cond(
        fits[0] == 1,
        lambda: shared_transform(layers, grids, *limits, fourier, weights, legendre, table, index),
        lambda: transform(layers, grids, fourier, weights, legendre, pair_slots),
    )
    return out.transpose(0, 2, 1)


def solution(mesh):
    in_specs = (P(("layer", "grid"), None, None), P(("layer", "grid")), P("grid", None, None), P())
    out_specs = P("grid", None, "layer")
    body = functools.partial(shards, mesh.shape["layer"], mesh.shape["grid"])
    return jax.shard_map(body, mesh=mesh, in_specs=in_specs, out_specs=out_specs, check_vma=False)
```

```python
import functools

import jax
import jax.numpy as jnp
from jax import lax
from jax.experimental import pallas as pl
from jax.experimental.pallas import tpu as pltpu
from jax.sharding import PartitionSpec as P

LANES = 128
SUBLANES = 8
MESH = pl.DeviceIdType.MESH


def split(x):
    high = x.astype(jnp.bfloat16)
    return high, (x - high.astype(jnp.float32)).astype(jnp.bfloat16)


def transform_kernel(
    layers, grids, waves, lats, chunk, ahead,
    slots_ref, w_ref, x_ref, poly_ref,
    o_ref, send_ref, recv_ref,
    scale, stage, poly, fields, result,
    load_sem, stage_sem, send_sem, recv_sem, poly_sem, field_sem, out_sem, *held,
):
    devices = layers * grids
    tiles, pitch = lats // SUBLANES, held[0].shape[0] // SUBLANES
    columns = len(held) // tiles
    local_pairs, half, degrees = o_ref.shape
    chunks = local_pairs // chunk
    per_group = SUBLANES // chunk
    my_layer, my_grid = lax.axis_index("layer"), lax.axis_index("grid")
    me = my_layer * grids + my_grid

    def loads(column, tile):
        for row in range(SUBLANES):
            yield pltpu.make_async_copy(
                x_ref.at[pl.ds((tile * SUBLANES + row) * waves, waves), pl.ds(column * LANES, LANES)],
                held[column * tiles + tile].at[pl.ds(row * pitch, waves)],
                load_sem.at[column, tile, row],
            )

    def poly_copies(group):
        rows = pl.ds(pl.multiple_of(group * SUBLANES, SUBLANES), SUBLANES)
        for part in range(poly.shape[0]):
            yield pltpu.make_async_copy(
                poly_ref.at[:, rows, pl.ds(part * LANES, LANES)],
                poly.at[part, pl.ds(0, degrees)],
                poly_sem.at[part],
            )

    def whole(ref, index, sem):
        block = ref.at[index, pl.ds(0, devices - 1)]
        return pltpu.make_async_copy(block, block, sem.at[index])

    for tile in range(tiles):
        for column in range(columns):
            for copy in loads(column, tile):
                copy.start()

    barrier = pltpu.get_barrier_semaphore()

    def greet(step, carry):
        other = lax.rem(me + step, devices)
        pl.semaphore_signal(
            barrier, inc=1, device_id=(other // grids, lax.rem(other, grids)), device_id_type=MESH
        )
        return carry

    lax.fori_loop(1, devices, greet, 0)

    row_ids = lax.broadcasted_iota(jnp.int32, (SUBLANES, LANES), 0)
    for tile in range(tiles):
        value = jnp.zeros((SUBLANES, LANES), jnp.float32)
        for row in range(SUBLANES):
            value = jnp.where(row_ids == row, w_ref[tile * SUBLANES + row], value)
        scale[tile] = value
    parts, rows = poly.shape[0], poly.shape[1]
    for part in range(parts):
        poly[part, pl.ds(degrees, rows - degrees)] = jnp.zeros((rows - degrees, SUBLANES, LANES), jnp.float32)

    in_low = lax.broadcasted_iota(jnp.int32, (SUBLANES, LANES), 1) < half

    def pack(index, first):
        for tile in range(tiles):
            for column in range(columns):
                if first:
                    for copy in loads(column, tile):
                        copy.wait()
                x = held[column * tiles + tile]
                weight = scale[tile]

                def step(q, carry):
                    grid, place = q // chunk, lax.rem(q, chunk)
                    a = slots_ref[grid * local_pairs + index * chunk + place]
                    one = x[pl.ds(a, SUBLANES, stride=pitch), :] * weight
                    two = x[pl.ds(waves - 1 - a, SUBLANES, stride=pitch), :] * weight
                    lower, upper = 2 * column * grids + grid, (2 * column + 1) * grids + grid
                    rows = pl.ds(tile * SUBLANES, SUBLANES)
                    stage[lower, place, rows] = jnp.where(in_low, one, pltpu.roll(two, half, 1))
                    stage[upper, place, rows] = jnp.where(in_low, pltpu.roll(one, half, 1), two)
                    return carry

                lax.fori_loop(0, grids * chunk, step, 0, unroll=8)
        out = pltpu.make_async_copy(stage, send_ref.at[index], stage_sem.at[0])
        own = pltpu.make_async_copy(stage.at[me], recv_ref.at[index, me], stage_sem.at[1])
        out.start()
        own.start()
        out.wait()
        own.wait()

    def send(index):
        def step(k, carry):
            other = lax.rem(me + k, devices)
            pltpu.make_async_remote_copy(
                src_ref=send_ref.at[index, other],
                dst_ref=recv_ref.at[index, me],
                send_sem=send_sem.at[index],
                recv_sem=recv_sem.at[index],
                device_id=(other // grids, lax.rem(other, grids)),
                device_id_type=MESH,
            ).start()
            return carry

        lax.fori_loop(1, devices, step, 0)

    pack(0, True)
    pl.semaphore_wait(barrier, devices - 1)
    send(0)
    for copy in poly_copies(0):
        copy.start()

    def prepare(index, carry):
        pack(index, False)
        send(index)
        return carry

    lax.fori_loop(1, ahead, prepare, 0)

    def consume(index, carry):
        @pl.when(index + ahead < chunks)
        def _():
            prepare(index + ahead, 0)

        group, place = index // per_group, lax.rem(index, per_group)

        @pl.when(place == 0)
        def _():
            for copy in poly_copies(group):
                copy.wait()

        whole(recv_ref, index, recv_sem).wait()
        copy = pltpu.make_async_copy(recv_ref.at[index], fields, field_sem)
        copy.start()
        copy.wait()

        def pair(p, carry):
            limit = waves - slots_ref[my_grid * local_pairs + index * chunk + p]
            x = fields[:, pl.ds(p, 1)].reshape(devices * lats, LANES)
            right = jnp.concatenate(split(x), axis=1)
            spots = pl.ds(place * chunk + p, rows, stride=SUBLANES)
            left = [poly.at[part].reshape(rows * SUBLANES, LANES)[spots, :] for part in range(parts)]
            high, low = split(jnp.concatenate(left, axis=1))
            product = jnp.dot(high, right, preferred_element_type=jnp.float32)
            product = product + jnp.dot(low, right, preferred_element_type=jnp.float32)
            total = (product[:, :LANES] + product[:, LANES:]).T
            ids = lax.broadcasted_iota(jnp.int32, (half, rows), 1)
            result[p] = jnp.where(ids < limit, total[:half], total[half:])[:, :degrees]
            return carry

        lax.fori_loop(0, chunk, pair, 0)

        @pl.when((place == per_group - 1) & (index + 1 < chunks))
        def _():
            for copy in poly_copies(group + 1):
                copy.start()

        copy = pltpu.make_async_copy(result, o_ref.at[pl.ds(index * chunk, chunk)], out_sem)
        copy.start()
        copy.wait()
        return carry

    lax.fori_loop(0, chunks, consume, 0)

    def finish(index, carry):
        whole(send_ref, index, send_sem).wait()
        return carry

    lax.fori_loop(0, chunks, finish, 0)

def plan_kernel(grids, dropped, most, tallest, slots_ref, table_ref, index_ref, flag_ref):
    pairs = slots_ref.shape[0]
    waves, local_pairs = 2 * pairs, table_ref.shape[1]
    shape = (grids, local_pairs)
    lane = lax.broadcasted_iota(jnp.int32, shape, 1)
    code = lax.broadcasted_iota(jnp.int32, shape, 0) * local_pairs + lane
    zero = jnp.zeros(shape, jnp.int32)
    a = zero
    for p in range(pairs):
        a = jnp.where(code == p, slots_ref[p], a)
    b = waves - 1 - a
    rank = zero
    for p in range(local_pairs):
        rank = rank + jnp.where(a[:, p : p + 1] < a, 1, 0)
    kept = jnp.where(rank < dropped, 0, 1)
    place = zero
    for p in range(local_pairs):
        place = place + jnp.where(lane > p, kept[:, p : p + 1], 0)
    listed, gone, spot = zero, zero, zero
    for p in range(local_pairs):
        wave = b[:, p : p + 1]
        listed = listed + jnp.where((lane == place[:, p : p + 1]) & (kept[:, p : p + 1] == 1), wave, 0)
        mine = (lane == rank[:, p : p + 1]) & (lane < dropped)
        gone = gone + jnp.where(mine, wave, 0)
        spot = spot + jnp.where(mine, p, 0)
    count = jnp.where(lane < dropped, waves - gone, 0)
    end = zero
    for k in range(dropped):
        end = end + jnp.where(lane >= k, count[:, k : k + 1], 0)
    begin = end - count
    over = jnp.where((end > most) | (count > tallest), 1.0, 0.0)
    flag_ref[0] = (jnp.sum(over) < 0.5).astype(jnp.int32)
    place = jnp.where(kept == 1, place, 0)
    rank = jnp.where(kept == 1, 0, rank)
    bound = zero
    for k in range(dropped):
        bound = bound + jnp.where(rank == k, end[:, k : k + 1], 0)
    kinds = (a, listed, gone, place // 2, lax.rem(place, 2), kept, begin, end, bound)
    for index, value in enumerate(kinds):
        table_ref[pl.ds(index * grids, grids)] = value
    me = lax.axis_index("grid")

    def mine(value):
        row = jnp.zeros((1, local_pairs), jnp.int32)
        for grid in range(grids):
            row = row + jnp.where(grid == me, value[grid : grid + 1], 0)
        return row

    my_begin, my_end, my_spot = mine(begin), mine(end), mine(spot)
    slot = lax.broadcasted_iota(jnp.int32, index_ref.shape, 0) * LANES
    slot = slot + lax.broadcasted_iota(jnp.int32, index_ref.shape, 1)
    row = jnp.zeros(index_ref.shape, jnp.int32)
    for k in range(dropped):
        start, stop, place = my_begin[:, k : k + 1], my_end[:, k : k + 1], my_spot[:, k : k + 1]
        inside = (slot >= start) & (slot < stop)
        row = jnp.where(inside, (tallest - stop + slot) * local_pairs + place, row)
    index_ref[...] = jnp.maximum(row, 0)


KINDS = 9
SLOT, LISTED, GONE, LIST_TILE, LIST_SIDE, KEPT, BEGIN, END, BOUND = range(KINDS)


def plan(pair_slots, grids, dropped, most, tallest):
    return pl.pallas_call(
        functools.partial(plan_kernel, grids, dropped, most, tallest),
        in_specs=[pl.BlockSpec(memory_space=pltpu.SMEM)],
        out_specs=[pl.BlockSpec(memory_space=pltpu.VMEM)] * 2 + [pl.BlockSpec(memory_space=pltpu.SMEM)],
        out_shape=[
            jax.ShapeDtypeStruct((KINDS * grids, pair_slots.shape[0] // grids), jnp.int32),
            jax.ShapeDtypeStruct((pl.cdiv(most, LANES), LANES), jnp.int32),
            jax.ShapeDtypeStruct((1,), jnp.int32),
        ],
        name="plan",
    )(pair_slots)


def shared_kernel(
    layers, grids, waves, lats, dropped, tallest, ahead, help_at, wait_end,
    table_ref, index_ref, w_ref, x_ref, poly_ref,
    o_ref, send_ref, recv_ref, extra_out, extra_in, rows_out, rows_in, sums_out, sums_in,
    scale, stage, extra_stage, rows_tmp, rows_stage, poly, own, cross, listed, extra, far_rows, taken, sums, gathered, far_sums, result,
    load_sem, stage_sem, send_sem, recv_sem, poly_sem, field_sem, out_sem, extra_sems, rows_sems, sums_sems, *held,
):
    devices, side = layers * grids, grids // 2
    tiles, pitch = lats // SUBLANES, held[0].shape[0] // SUBLANES
    columns = len(held) // tiles
    local_pairs, half, degrees = o_ref.shape
    chunk = 2
    chunks = local_pairs // chunk
    full_chunks = (local_pairs - dropped) // chunk
    per_group = SUBLANES // chunk
    most = rows_out.shape[0]
    my_layer, my_grid = lax.axis_index("layer"), lax.axis_index("grid")
    me = my_layer * grids + my_grid
    my_side = my_grid // side
    partner = lax.rem(my_grid + side, grids)
    side_me = my_layer * side + lax.rem(my_grid, side)
    parts, rows = poly.shape[0], poly.shape[1]
    offset = rows - degrees

    def look(kind, grid, index):
        return table_ref[kind * grids + grid, index]

    def loads(column, tile):
        for row in range(SUBLANES):
            yield pltpu.make_async_copy(
                x_ref.at[pl.ds((tile * SUBLANES + row) * waves, waves), pl.ds(column * LANES, LANES)],
                held[column * tiles + tile].at[pl.ds(row * pitch, waves)],
                load_sem.at[column, tile, row],
            )

    def poly_copies(group):
        spots = pl.ds(pl.multiple_of(group * SUBLANES, SUBLANES), SUBLANES)
        for part in range(parts):
            yield pltpu.make_async_copy(
                poly_ref.at[:, spots, pl.ds(part * LANES, LANES)],
                poly.at[part, pl.ds(offset, degrees)],
                poly_sem.at[part],
            )

    far_lanes = pl.ds(pl.multiple_of((2 * my_layer + 1 - my_side) * LANES, LANES), LANES)
    rows_copy = pltpu.make_async_copy(
        poly_ref.at[pl.ds(degrees - tallest, tallest), :, far_lanes], rows_tmp, rows_sems.at[0]
    )
    rows_copy.start()
    for tile in range(tiles):
        for column in range(columns):
            for copy in loads(column, tile):
                copy.start()

    barrier = pltpu.get_barrier_semaphore()

    def greet(step, carry):
        other = lax.rem(me + step, devices)
        pl.semaphore_signal(
            barrier, inc=1, device_id=(other // grids, lax.rem(other, grids)), device_id_type=MESH
        )
        return carry

    lax.fori_loop(1, devices, greet, 0)

    row_ids = lax.broadcasted_iota(jnp.int32, (SUBLANES, LANES), 0)
    for tile in range(tiles):
        value = jnp.zeros((SUBLANES, LANES), jnp.float32)
        for row in range(SUBLANES):
            value = jnp.where(row_ids == row, w_ref[tile * SUBLANES + row], value)
        scale[tile] = value
    for part in range(parts):
        poly[part, pl.ds(0, offset)] = jnp.zeros((offset, SUBLANES, LANES), jnp.float32)
    sums[pl.ds(0, tallest)] = jnp.zeros((tallest, LANES), jnp.float32)

    rows_send = pltpu.make_async_remote_copy(
        src_ref=rows_out,
        dst_ref=rows_in.at[my_layer],
        send_sem=rows_sems.at[1],
        recv_sem=rows_sems.at[2],
        device_id=(my_layer, partner),
        device_id_type=MESH,
    )

    def send_rows():
        rows_copy.wait()
        flat_rows = rows_tmp.reshape(tallest * local_pairs, LANES)

        def pick(t, carry):
            row = index_ref[t // LANES, lax.rem(t, LANES)]
            rows_stage[pl.ds(t, 1)] = flat_rows[pl.ds(row, 1), :]
            return carry

        lax.fori_loop(0, most, pick, 0, unroll=16)

        keep = pltpu.make_async_copy(rows_stage, rows_out, rows_sems.at[0])
        keep.start()
        keep.wait()
        rows_send.start()

    in_low = lax.broadcasted_iota(jnp.int32, (SUBLANES, LANES), 1) < half

    def gather(count, waves_of, target, first):
        for tile in range(tiles):
            for column in range(columns):
                if first:
                    for copy in loads(column, tile):
                        copy.wait()
                x = held[column * tiles + tile]
                weight = scale[tile]

                def step(q, carry):
                    one_wave, two_wave, grid, place = waves_of(q)
                    one = x[pl.ds(one_wave, SUBLANES, stride=pitch), :] * weight
                    two = x[pl.ds(two_wave, SUBLANES, stride=pitch), :] * weight
                    span = target.shape[0] // layers
                    lower, upper = 2 * column * span + grid, (2 * column + 1) * span + grid
                    spots = pl.ds(tile * SUBLANES, SUBLANES)
                    target[lower, place, spots] = jnp.where(in_low, one, pltpu.roll(two, half, 1))
                    target[upper, place, spots] = jnp.where(in_low, pltpu.roll(one, half, 1), two)
                    return carry

                lax.fori_loop(0, count, step, 0, unroll=8)

    def put(target, out, kept, here):
        one = pltpu.make_async_copy(target, out, stage_sem.at[0])
        two = pltpu.make_async_copy(target.at[here], kept, stage_sem.at[1])
        one.start()
        two.start()
        one.wait()
        two.wait()

    def pack(index, first):
        def waves_of(q):
            grid, place = q // chunk, lax.rem(q, chunk)
            across = grid // side != my_side
            head = place == 0
            a0, a1 = look(SLOT, grid, index * chunk), look(SLOT, grid, index * chunk + 1)
            b0, b1 = look(LISTED, grid, index * chunk), look(LISTED, grid, index * chunk + 1)
            a = jnp.where(head, a0, a1)
            one = jnp.where(across, jnp.where(head, a0, b0), a)
            two = jnp.where(across, jnp.where(head, a1, b1), waves - 1 - a)
            return one, two, grid, place

        gather(grids * chunk, waves_of, stage, first)
        put(stage, send_ref.at[index], recv_ref.at[index, me], me)

    def send(index):
        def start(k, which, count):
            place = lax.rem(side_me + k, layers * side)
            layer, grid = place // side, which * side + lax.rem(place, side)
            pltpu.make_async_remote_copy(
                src_ref=send_ref.at[index, layer * grids + grid, pl.ds(0, count)],
                dst_ref=recv_ref.at[index, me, pl.ds(0, count)],
                send_sem=send_sem.at[index],
                recv_sem=recv_sem.at[index],
                device_id=(layer, grid),
                device_id_type=MESH,
            ).start()

        def far(k, carry):
            @pl.when(index < full_chunks)
            def _():
                start(k, 1 - my_side, 2)

            @pl.when(index >= full_chunks)
            def _():
                start(k, 1 - my_side, 1)

            return carry

        def near(k, carry):
            start(k, my_side, 2)
            return carry

        lax.fori_loop(0, layers * side, far, 0)
        lax.fori_loop(1, layers * side, near, 0)

    def whole(ref, index, sem):
        @pl.when(index < full_chunks)
        def _():
            block = ref.at[index, pl.ds(0, devices - 1)]
            pltpu.make_async_copy(block, block, sem.at[index]).wait()

        @pl.when(index >= full_chunks)
        def _():
            block = ref.at[index, pl.ds(0, 3 * devices // 4 - 1)]
            pltpu.make_async_copy(block, block, sem.at[index]).wait()

    def extra_wait(ref, sem):
        block = ref.at[pl.ds(0, layers * side - 1)]
        pltpu.make_async_copy(block, block, sem).wait()

    def send_extra():
        def waves_of(q):
            grid, place = q // (dropped // 2), lax.rem(q, dropped // 2)
            owner = lax.rem((1 - my_side) * side + grid, grids)
            return look(GONE, owner, 2 * place), look(GONE, owner, 2 * place + 1), grid, place

        gather(side * dropped // 2, waves_of, extra_stage, False)
        put(extra_stage, extra_out, extra_in.at[side_me], side_me)

        def step(k, carry):
            other = lax.rem(side_me + k, layers * side)
            pltpu.make_async_remote_copy(
                src_ref=extra_out.at[other],
                dst_ref=extra_in.at[side_me],
                send_sem=extra_sems.at[0],
                recv_sem=extra_sems.at[1],
                device_id=(other // side, my_side * side + lax.rem(other, side)),
                device_id_type=MESH,
            ).start()
            return carry

        lax.fori_loop(1, layers * side, step, 0)

    def forward():
        rows_send.wait_recv()

        def step(k, carry):
            pltpu.make_async_remote_copy(
                src_ref=rows_in.at[my_layer],
                dst_ref=rows_in.at[my_layer],
                send_sem=rows_sems.at[3],
                recv_sem=rows_sems.at[4],
                device_id=(lax.rem(my_layer + k, layers), my_grid),
                device_id_type=MESH,
            ).start()
            return carry

        lax.fori_loop(1, layers, step, 0)

    def forward_wait(sem):
        block = rows_in.at[pl.ds(0, layers - 1)]
        pltpu.make_async_copy(block, block, sem).wait()

    sums_send = pltpu.make_async_remote_copy(
        src_ref=sums_out,
        dst_ref=sums_in,
        send_sem=sums_sems.at[0],
        recv_sem=sums_sems.at[1],
        device_id=(my_layer, partner),
        device_id_type=MESH,
    )

    def multiply(left, right):
        right = jnp.concatenate(split(right), axis=1)
        high, low = split(left)
        product = jnp.dot(high, right, preferred_element_type=jnp.float32)
        product = product + jnp.dot(low, right, preferred_element_type=jnp.float32)
        return product[:, :LANES] + product[:, LANES:]

    def help_partner():
        extra_wait(extra_in, extra_sems.at[1])
        forward_wait(rows_sems.at[4])
        one = pltpu.make_async_copy(extra_in, extra, field_sem.at[0, 0])
        two = pltpu.make_async_copy(rows_in, far_rows, field_sem.at[1, 0])
        one.start()
        two.start()
        one.wait()
        two.wait()
        gathered[...] = jnp.zeros(gathered.shape, jnp.float32)
        ids = lax.broadcasted_iota(jnp.int32, (most, LANES), 0)
        low = lax.broadcasted_iota(jnp.int32, (most, LANES), 1) < half

        def tile(index, carry):
            right = extra[:, pl.ds(index, 1)].reshape(layers * side * lats, LANES)
            left = jnp.concatenate([far_rows[layer] for layer in range(layers)], axis=1)
            first, last = look(BEGIN, partner, 2 * index), look(END, partner, 2 * index)
            limit = look(END, partner, 2 * index + 1)
            start = jnp.where(low, first, last)
            stop = jnp.where(low, last, limit)
            gathered[...] += jnp.where((ids >= start) & (ids < stop), multiply(left, right), 0.0)
            return carry

        lax.fori_loop(0, dropped // 2, tile, 0)
        value = gathered[...]
        value = value + pltpu.roll(value, half, 1)
        low = lax.broadcasted_iota(jnp.int32, (most // 2, LANES), 1) < half
        far_sums[...] = jnp.where(low, value[: most // 2], value[most // 2 :])
        copy = pltpu.make_async_copy(far_sums, sums_out, field_sem.at[0, 0])
        copy.start()
        copy.wait()
        sums_send.start()

    def take_sums():
        sums_send.wait_recv()
        copy = pltpu.make_async_copy(sums_in, taken, sums_sems.at[2])
        copy.start()
        copy.wait()
        value = taken[...]
        sums[pl.ds(tallest, most // 2)] = pltpu.roll(value, half, 1)
        sums[pl.ds(tallest + most // 2, most // 2)] = value

    pack(0, True)
    pl.semaphore_wait(barrier, devices - 1)
    send(0)
    send_rows()
    send_extra()
    for copy in poly_copies(0):
        copy.start()

    def prepare(index, carry):
        pack(index, False)

        @pl.when(index < ahead)
        def _():
            send(index)

        return carry

    pause = (ahead + chunks) // 2
    lax.fori_loop(1, pause, prepare, 0)
    forward()
    lax.fori_loop(pause, chunks, prepare, 0)

    def arrive(index, carry):
        @pl.when(index + ahead < chunks)
        def _():
            send(index + ahead)

        whole(recv_ref, index, recv_sem)
        return carry

    def consume(index, carry):
        group, place = index // per_group, lax.rem(index, per_group)

        @pl.when(place == 0)
        def _():
            for copy in poly_copies(group):
                copy.wait()

        near, far = my_side * side, (1 - my_side) * side
        copies = []
        for layer in range(layers):
            copies.append(
                pltpu.make_async_copy(
                    recv_ref.at[index, pl.ds(layer * grids + near, side)], own.at[layer], field_sem.at[0, layer]
                )
            )
            copies.append(
                pltpu.make_async_copy(
                    recv_ref.at[index, pl.ds(layer * grids + far, side), 0], cross.at[layer], field_sem.at[1, layer]
                )
            )
        lists = [
            pltpu.make_async_copy(
                recv_ref.at[index, pl.ds(layer * grids + far, side), 1], listed.at[index, layer], field_sem.at[2, layer]
            )
            for layer in range(layers)
        ]

        @pl.when(index < full_chunks)
        def _():
            for copy in lists:
                copy.start()

        for copy in copies:
            copy.start()
        for copy in copies:
            copy.wait()

        @pl.when(index < full_chunks)
        def _():
            for copy in lists:
                copy.wait()

        def pair(p, carry):
            q = index * chunk + p
            limit = waves - look(SLOT, my_grid, q)
            block = (layers * side * lats, LANES)
            near_x = own[:, :, pl.ds(p, 1)].reshape(block)
            low = lax.broadcasted_iota(jnp.int32, block, 1) < half
            first = cross[...].reshape(block)
            first = jnp.where(p == 0, first, pltpu.roll(first, half, 1))
            second = listed[pl.ds(look(LIST_TILE, my_grid, q), 1)].reshape(block)
            second = jnp.where(look(LIST_SIDE, my_grid, q) == 1, second, pltpu.roll(second, half, 1))
            keep = look(KEPT, my_grid, q)
            second = jnp.where(keep == 1, second, 0.0)
            right = jnp.concatenate([near_x, jnp.where(low, first, second)], axis=0)
            spots = pl.ds(place * chunk + p, rows, stride=SUBLANES)
            order = [2 * layer + my_side for layer in range(layers)]
            order += [2 * layer + 1 - my_side for layer in range(layers)]
            left = [poly.at[part].reshape(rows * SUBLANES, LANES)[spots, :] for part in order]
            product = multiply(jnp.concatenate(left, axis=1), right)
            more = sums[pl.ds(look(BOUND, my_grid, q), tallest), :]
            high = lax.broadcasted_iota(jnp.int32, more.shape, 1) >= half
            more = jnp.where(high & (keep == 0), more, 0.0)
            product = jnp.concatenate([product[: rows - tallest], product[rows - tallest :] + more], axis=0)
            total = product.T
            ids = lax.broadcasted_iota(jnp.int32, (half, rows), 1) - offset
            result[p] = jnp.where(ids < limit, total[:half], total[half:])[:, offset:]
            return carry

        lax.fori_loop(0, chunk, pair, 0, unroll=True)

        @pl.when((place == per_group - 1) & (index + 1 < chunks))
        def _():
            for copy in poly_copies(group + 1):
                copy.start()

        copy = pltpu.make_async_copy(result, o_ref.at[pl.ds(index * chunk, chunk)], out_sem)
        copy.start()
        copy.wait()
        return carry

    def step(index, carry):
        arrive(index, 0)
        late = index - wait_end
        begin = jnp.where(late < wait_end, 2 * late, index)
        end = jnp.where(late < wait_end, 2 * late + 2, index + 1)
        return lax.fori_loop(begin, end, consume, 0)

    lax.fori_loop(0, help_at, arrive, 0)
    help_partner()
    lax.fori_loop(help_at, wait_end, arrive, 0)
    take_sums()
    lax.fori_loop(wait_end, chunks, step, 0)

    def finish(index, carry):
        whole(send_ref, index, send_sem)
        return carry

    lax.fori_loop(0, chunks, finish, 0)
    rows_send.wait_send()
    sums_send.wait_send()
    forward_wait(rows_sems.at[3])
    extra_wait(extra_out, extra_sems.at[0])


def shared_transform(layers, grids, dropped, most, tallest, fourier, weights, legendre, table, index):
    local_pairs, degrees, all_lats = legendre.shape
    lats, waves, all_fields = fourier.shape
    half = all_fields // layers
    devices, side, count = layers * grids, grids // 2, dropped // 2
    chunk = 2
    chunks = local_pairs // chunk
    ahead = min(3, chunks)
    help_at, wait_end = max(1, chunks // 8), max(1, chunks * 5 // 16)
    rows = (degrees + SUBLANES - 1) // SUBLANES * SUBLANES
    columns, tiles, pitch = all_fields // LANES, lats // SUBLANES, waves + SUBLANES
    block = (devices, chunk, lats, LANES)
    near = (layers * side, count, lats, LANES)
    hbm = pl.BlockSpec(memory_space=pl.ANY)
    smem = pl.BlockSpec(memory_space=pltpu.SMEM)

    def shape(*sizes):
        return jax.ShapeDtypeStruct(sizes, jnp.float32)

    def vmem(*sizes):
        return pltpu.VMEM(sizes, jnp.float32)

    return pl.pallas_call(
        functools.partial(shared_kernel, layers, grids, waves, lats, dropped, tallest, ahead, help_at, wait_end),
        in_specs=[smem, smem, smem, hbm, hbm],
        out_specs=[hbm] * 9,
        out_shape=[
            shape(local_pairs, half, degrees),
            shape(chunks, *block),
            shape(chunks, *block),
            shape(*near),
            shape(*near),
            shape(most, LANES),
            shape(layers, most, LANES),
            shape(most // 2, LANES),
            shape(most // 2, LANES),
        ],
        scratch_shapes=[
            vmem(tiles, SUBLANES, LANES),
            vmem(*block),
            vmem(*near),
            vmem(tallest, local_pairs, LANES),
            vmem(most, LANES),
            vmem(all_lats // LANES, rows, SUBLANES, LANES),
            vmem(layers, side, chunk, lats, LANES),
            vmem(layers, side, lats, LANES),
            vmem((local_pairs - dropped) // chunk, layers, side, lats, LANES),
            vmem(*near),
            vmem(layers, most, LANES),
            vmem(most // 2, LANES),
            vmem(tallest + most, LANES),
            vmem(most, LANES),
            vmem(most // 2, LANES),
            vmem(chunk, half, degrees),
            pltpu.SemaphoreType.DMA((columns, tiles, SUBLANES)),
            pltpu.SemaphoreType.DMA((2,)),
            pltpu.SemaphoreType.DMA((chunks,)),
            pltpu.SemaphoreType.DMA((chunks,)),
            pltpu.SemaphoreType.DMA((all_lats // LANES,)),
            pltpu.SemaphoreType.DMA((3, layers)),
            pltpu.SemaphoreType.DMA,
            pltpu.SemaphoreType.DMA((2,)),
            pltpu.SemaphoreType.DMA((5,)),
            pltpu.SemaphoreType.DMA((3,)),
        ]
        + [vmem(SUBLANES * pitch, LANES)] * (columns * tiles),
        compiler_params=pltpu.CompilerParams(
            collective_id=1, has_side_effects=True, vmem_limit_bytes=63 * 2**20
        ),
        name="shared",
    )(table, index, weights, fourier.reshape(lats * waves, all_fields), legendre.transpose(1, 0, 2))[0]


def row_limits(pairs, local_pairs):
    dropped = max(2, local_pairs * 3 // 8 // 2 * 2)
    shares = [k / (local_pairs + 1) for k in range(1, dropped + 1)]
    means = [(pairs + 1) * share for share in shares]
    spreads = [(pairs + 1) * (share * (1 - share) / (local_pairs + 2)) ** 0.5 for share in shares]
    most = int(sum(means) + 2.6 * sum(spreads) + 15) // 16 * 16
    tallest = int(means[-1] + 3.1 * spreads[-1] + 7) // 8 * 8
    return dropped, most, min(tallest, pairs)


def transform(layers, grids, fourier, weights, legendre, pair_slots):
    local_pairs, degrees, all_lats = legendre.shape
    waves = 2 * pair_slots.shape[0]
    lats, _, all_fields = fourier.shape
    half = all_fields // layers
    devices = layers * grids
    chunk = 2
    chunks = local_pairs // chunk
    ahead = min(3, chunks)
    rows = (degrees + SUBLANES - 1) // SUBLANES * SUBLANES
    columns, tiles, pitch = all_fields // LANES, lats // SUBLANES, waves + SUBLANES
    block = (devices, chunk, lats, LANES)
    hbm = pl.BlockSpec(memory_space=pl.ANY)
    smem = pl.BlockSpec(memory_space=pltpu.SMEM)
    return pl.pallas_call(
        functools.partial(transform_kernel, layers, grids, waves, lats, chunk, ahead),
        in_specs=[smem, smem, hbm, hbm],
        out_specs=[hbm, hbm, hbm],
        out_shape=[
            jax.ShapeDtypeStruct((local_pairs, half, degrees), jnp.float32),
            jax.ShapeDtypeStruct((chunks,) + block, jnp.float32),
            jax.ShapeDtypeStruct((chunks,) + block, jnp.float32),
        ],
        scratch_shapes=[
            pltpu.VMEM((tiles, SUBLANES, LANES), jnp.float32),
            pltpu.VMEM(block, jnp.float32),
            pltpu.VMEM((all_lats // LANES, rows, SUBLANES, LANES), jnp.float32),
            pltpu.VMEM(block, jnp.float32),
            pltpu.VMEM((chunk, half, degrees), jnp.float32),
            pltpu.SemaphoreType.DMA((columns, tiles, SUBLANES)),
            pltpu.SemaphoreType.DMA((2,)),
            pltpu.SemaphoreType.DMA((chunks,)),
            pltpu.SemaphoreType.DMA((chunks,)),
            pltpu.SemaphoreType.DMA((all_lats // LANES,)),
            pltpu.SemaphoreType.DMA,
            pltpu.SemaphoreType.DMA,
        ]
        + [pltpu.VMEM((SUBLANES * pitch, LANES), jnp.float32)] * (columns * tiles),
        compiler_params=pltpu.CompilerParams(
            collective_id=0, has_side_effects=True, vmem_limit_bytes=60 * 2**20
        ),
        name="transform",
    )(pair_slots, weights, fourier.reshape(lats * waves, all_fields), legendre.transpose(1, 0, 2))[0]


def shards(layers, grids, fourier, weights, legendre, pair_slots):
    pairs, local_pairs = pair_slots.shape[0], legendre.shape[0]
    limits = row_limits(pairs, local_pairs)
    table, index, fits = plan(pair_slots, grids, *limits)
    out = lax.cond(
        fits[0] == 1,
        lambda: shared_transform(layers, grids, *limits, fourier, weights, legendre, table, index),
        lambda: transform(layers, grids, fourier, weights, legendre, pair_slots),
    )
    return out.transpose(0, 2, 1)


def solution(mesh):
    in_specs = (P(("layer", "grid"), None, None), P(("layer", "grid")), P("grid", None, None), P())
    out_specs = P("grid", None, "layer")
    body = functools.partial(shards, mesh.shape["layer"], mesh.shape["grid"])
    return jax.shard_map(body, mesh=mesh, in_specs=in_specs, out_specs=out_specs, check_vma=False)
```
